32 devices in a mesh: stage: 4 (over z), expert: 8 (over y, x, core).
Axes of the slice: x: 2, y: 2, z: 4, core: 2. Of those that a mesh axis runs over, the one named last changes fastest.
Arguments:
- tokens_in: bfloat16 [4, 8192, 1024], P('stage', 'expert')
- expert_ids: int32 [4, 8192, 8], P('stage', 'expert')
- gate_wts: float32 [4, 8192, 8], P('stage', 'expert')
- w_gate: bfloat16 [4, 32, 1024, 512], P('stage', 'expert')
- w_up: bfloat16 [4, 32, 1024, 512], P('stage', 'expert')
- w_down: bfloat16 [4, 32, 512, 1024], P('stage', 'expert')
- grad_out: bfloat16 [4, 8192, 1024], P('stage', 'expert')
Outputs:
- output 1: bfloat16 [4, 8192, 1024], P('stage', 'expert')
- output 2: bfloat16 [4, 8192, 1024], P('stage', 'expert')
- output 3: bfloat16 [4, 32, 1024, 512], P('stage', 'expert')
- output 4: bfloat16 [4, 32, 1024, 512], P('stage', 'expert')
- output 5: bfloat16 [4, 32, 512, 1024], P('stage', 'expert')
All inputs are finite; a program needn't handle non-finite values.
Results may differ from the reference program's by a relative error of at most 0.00782445.
Values are sent between devices in bfloat16 or wider.
A program may use at most 1 GiB of HBM per device.

```python
import jax
import jax.numpy as jnp
from jax import lax

STAGE_SIZE = 4
GROUP_SIZE = 8
TOKENS_DEV = 1024
D_MODEL = 1024
D_FF = 512
EXPERTS = 32
TOP_K = 8

HALF_STAGE = STAGE_SIZE // 2
LANE_TOKENS = GROUP_SIZE * TOKENS_DEV
CAPACITY = 3 * TOKENS_DEV * TOP_K // (2 * EXPERTS)


def route_source(src_key):
    key_perm, key_pair, key_tok = jax.random.split(src_key, 3)
    base_count = TOKENS_DEV * TOP_K // EXPERTS
    half_count = base_count // 2
    run_order = jax.random.permutation(key_perm, EXPERTS)
    pair_shift = jax.random.randint(key_pair, (EXPERTS // 2,), 0, half_count + 1)
    pair_shift = pair_shift.at[0].set(half_count)
    counts = jnp.stack([base_count + pair_shift, base_count - pair_shift], axis=1).reshape(EXPERTS)
    run_ends = jnp.cumsum(counts)
    tok_perm = jax.random.permutation(key_tok, TOKENS_DEV)
    flat_pos = tok_perm[:, None] + TOKENS_DEV * jnp.arange(TOP_K)[None, :]
    run_ids = jnp.searchsorted(run_ends, flat_pos, side="right")
    return run_order[run_ids].astype(jnp.int32)


def setup_inputs(seed: int = 0) -> dict:
    key_list = jax.random.split(jax.random.key(seed), 7)
    tok_shape = (STAGE_SIZE, LANE_TOKENS, D_MODEL)
    tokens_in = jax.random.normal(key_list[0], tok_shape, jnp.float32)
    src_keys = jax.random.split(key_list[1], STAGE_SIZE * GROUP_SIZE)
    expert_ids = jax.vmap(route_source)(src_keys).reshape(STAGE_SIZE, LANE_TOKENS, TOP_K)
    gate_wts = jax.random.uniform(key_list[2], (STAGE_SIZE, LANE_TOKENS, TOP_K), jnp.float32, 0.5, 1.5) * TOP_K ** -0.5
    w_gate = jax.random.normal(key_list[3], (STAGE_SIZE, EXPERTS, D_MODEL, D_FF), jnp.float32) * D_MODEL ** -0.5
    w_up = jax.random.normal(key_list[4], (STAGE_SIZE, EXPERTS, D_MODEL, D_FF), jnp.float32) * D_MODEL ** -0.5
    w_down = jax.random.normal(key_list[5], (STAGE_SIZE, EXPERTS, D_FF, D_MODEL), jnp.float32) * D_FF ** -0.5
    grad_out = jax.random.normal(key_list[6], tok_shape, jnp.float32)
    return {
        "tokens_in": tokens_in.astype(jnp.bfloat16),
        "expert_ids": expert_ids,
        "gate_wts": gate_wts,
        "w_gate": w_gate.astype(jnp.bfloat16),
        "w_up": w_up.astype(jnp.bfloat16),
        "w_down": w_down.astype(jnp.bfloat16),
        "grad_out": grad_out.astype(jnp.bfloat16),
    }


def lane_pass(lane_in):
    tokens, expert_ids, gate_wts, w_gate, w_up, w_down, grad_out = lane_in
    asg_count = LANE_TOKENS * TOP_K
    buf_rows = GROUP_SIZE * CAPACITY
    flat_ids = expert_ids.reshape(asg_count)
    tok_pad = jnp.concatenate([tokens, jnp.zeros((1, D_MODEL), tokens.dtype)], axis=0)
    dy_pad = jnp.concatenate([grad_out, jnp.zeros((1, D_MODEL), grad_out.dtype)], axis=0)
    gate_pad = jnp.concatenate([gate_wts.reshape(asg_count), jnp.zeros((1,), jnp.float32)])

    def expert_step(carry, expert_in):
        y_acc, dx_acc = carry
        expert_num, w_gate_e, w_up_e, w_down_e = expert_in
        is_hit = (flat_ids == expert_num).astype(jnp.int32)
        buf_pos = jnp.where(is_hit > 0, jnp.cumsum(is_hit) - 1, buf_rows)
        asg_row = jnp.full((buf_rows,), asg_count, jnp.int32).at[buf_pos].set(jnp.arange(asg_count, dtype=jnp.int32), mode="drop")
        tok_row = asg_row // TOP_K
        x_rows = tok_pad[tok_row]
        gate_row = gate_pad[asg_row]
        pre_gate = jnp.dot(x_rows, w_gate_e, preferred_element_type=jnp.float32)
        pre_up = jnp.dot(x_rows, w_up_e, preferred_element_type=jnp.float32)
        sig_gate = jax.nn.sigmoid(pre_gate)
        act_gate = pre_gate * sig_gate
        hidden = (act_gate * pre_up).astype(jnp.bfloat16)
        out_rows = jnp.dot(hidden, w_down_e, preferred_element_type=jnp.float32).astype(jnp.bfloat16)
        y_acc = y_acc + jax.ops.segment_sum(gate_row[:, None] * out_rows.astype(jnp.float32), tok_row, num_segments=LANE_TOKENS + 1)
        g_out = (gate_row[:, None] * dy_pad[tok_row].astype(jnp.float32)).astype(jnp.bfloat16)
        d_hidden = jnp.dot(g_out, w_down_e.T, preferred_element_type=jnp.float32)
        d_gate = (d_hidden * pre_up * sig_gate * (1.0 + pre_gate * (1.0 - sig_gate))).astype(jnp.bfloat16)
        d_up = (d_hidden * act_gate).astype(jnp.bfloat16)
        dx_rows = (jnp.dot(d_gate, w_gate_e.T, preferred_element_type=jnp.float32) + jnp.dot(d_up, w_up_e.T, preferred_element_type=jnp.float32)).astype(jnp.bfloat16)
        dx_acc = dx_acc + jax.ops.segment_sum(dx_rows.astype(jnp.float32), tok_row, num_segments=LANE_TOKENS + 1)
        grad_wg = jnp.dot(x_rows.T, d_gate, preferred_element_type=jnp.float32).astype(jnp.bfloat16)
        grad_wu = jnp.dot(x_rows.T, d_up, preferred_element_type=jnp.float32).astype(jnp.bfloat16)
        grad_wd = jnp.dot(hidden.T, g_out, preferred_element_type=jnp.float32).astype(jnp.bfloat16)
        return (y_acc, dx_acc), (grad_wg, grad_wu, grad_wd)

    zero_acc = jnp.zeros((LANE_TOKENS + 1, D_MODEL), jnp.float32)
    expert_in = (jnp.arange(EXPERTS, dtype=jnp.int32), w_gate, w_up, w_down)
    (y_acc, dx_acc), (grad_wg, grad_wu, grad_wd) = lax.scan(expert_step, (zero_acc, zero_acc), expert_in)
    return y_acc[:LANE_TOKENS].astype(jnp.bfloat16), dx_acc[:LANE_TOKENS].astype(jnp.bfloat16), grad_wg, grad_wu, grad_wd


def reference(tokens_in, expert_ids, gate_wts, w_gate, w_up, w_down, grad_out):
    lane_in = (
        tokens_in[:HALF_STAGE],
        expert_ids[:HALF_STAGE],
        gate_wts[:HALF_STAGE],
        w_gate[HALF_STAGE:],
        w_up[HALF_STAGE:],
        w_down[HALF_STAGE:],
        grad_out[HALF_STAGE:],
    )
    y_b, dx_a, grad_wg, grad_wu, grad_wd = lax.map(lane_pass, lane_in)
    y_out = jnp.concatenate([jnp.zeros_like(y_b), y_b], axis=0)
    grad_tokens = jnp.concatenate([dx_a, jnp.zeros_like(dx_a)], axis=0)
    grad_w_gate = jnp.concatenate([jnp.zeros_like(grad_wg), grad_wg], axis=0)
    grad_w_up = jnp.concatenate([jnp.zeros_like(grad_wu), grad_wu], axis=0)
    grad_w_down = jnp.concatenate([jnp.zeros_like(grad_wd), grad_wd], axis=0)
    return (y_out, grad_tokens, grad_w_gate, grad_w_up, grad_w_down)
```

```python
import functools

import jax
import jax.numpy as jnp
from jax import lax
from jax.experimental import pallas as pl
from jax.experimental.pallas import tpu as pltpu
from jax.sharding import PartitionSpec as P

MESH = pl.DeviceIdType.MESH
ANY = pl.BlockSpec(memory_space=pl.ANY)
F32 = jnp.float32
BF16 = jnp.bfloat16


def flip(ex, mask):
    bit_y = (ex // 4 + mask // 4) % 2
    bit_x = (ex // 2 + mask // 2) % 2
    bit_c = (ex + mask) % 2
    return bit_y * 4 + bit_x * 2 + bit_c


def dot(lhs, rhs, lhs_dim, rhs_dim):
    return lax.dot_general(lhs, rhs, (((lhs_dim,), (rhs_dim,)), ((), ())), preferred_element_type=F32)


AG_KINDS = (
    ((0, 1, 1), (0, 1, 1)),
    ((0, 2, 2), (0, 2, 2)),
    ((0, 4, 4), (0, 4, 4)),
    ((2, 1, 3), (2, 1, 3)),
    ((4, 1, 5), (4, 1, 5)),
    ((2, 4, 6), (4, 2, 6)),
    ((6, 1, 7), (6, 1, 7)),
)
K_OWN_P, K_OWN_X, K_OWN_Y, K_FWD_X, K_FWD_Y, K_DIAG, K_FWD_D = range(7)


def gather_kernel(n_half, x_ref, dy_ref, g_ref, xall, dyall, gall, own_buf, send_sem, recv_sem, z_send, z_recv, g_send, g_recv, loc_sem):
    st = lax.axis_index("stage")
    ex = lax.axis_index("expert")
    tok = x_ref.shape[0]
    rows_half = tok // 2
    bar = pltpu.get_barrier_semaphore()

    def block(arr, mask, half):
        start = pl.multiple_of(flip(ex, mask) * tok + half * rows_half, rows_half)
        return arr.at[pl.ds(start, rows_half)]

    def z_copy(half):
        return pltpu.make_async_remote_copy(
            src_ref=x_ref.at[pl.ds(half * rows_half, rows_half)], dst_ref=block(xall, 0, half),
            send_sem=z_send.at[half], recv_sem=z_recv.at[half], device_id=(st + n_half, ex), device_id_type=MESH)

    def zg_copy():
        return pltpu.make_async_remote_copy(
            src_ref=g_ref, dst_ref=gall.at[ex], send_sem=z_send.at[2], recv_sem=z_recv.at[2],
            device_id=(st + n_half, ex), device_id_type=MESH)

    @pl.when(st < n_half)
    def _():
        pl.semaphore_signal(bar, inc=1, device_id=(st + n_half, ex), device_id_type=MESH)
        pl.semaphore_wait(bar, 1)
        copies = [zg_copy(), z_copy(0), z_copy(1)]
        for c in copies:
            c.start()
        for c in copies:
            c.wait_send()

    @pl.when(st >= n_half)
    def _():
        pl.semaphore_signal(bar, inc=1, device_id=(st - n_half, ex), device_id_type=MESH)
        for mask in range(1, 8):
            pl.semaphore_signal(bar, inc=1, device_id=(st, flip(ex, mask)), device_id_type=MESH)
        pl.semaphore_wait(bar, 8)

        def copy(arr_id, kind, half, incoming=False):
            arr = (xall, dyall)[arr_id]
            sent, target, got = AG_KINDS[kind][half]
            sem = (arr_id * 7 + kind) * 2 + half
            dst = block(arr, got if incoming else sent, half)
            src = dst
            if sent == 0 and arr_id == 1 and not incoming:
                src = dy_ref.at[pl.ds(half * rows_half, rows_half)]
            return pltpu.make_async_remote_copy(
                src_ref=src, dst_ref=dst, send_sem=send_sem.at[sem], recv_sem=recv_sem.at[sem],
                device_id=(st, flip(ex, target)), device_id_type=MESH)

        def got(arr_id, kind, half):
            copy(arr_id, kind, half, incoming=True).wait_recv()

        def own(arr_id, half):
            for kind in (K_OWN_X, K_OWN_Y, K_OWN_P):
                copy(arr_id, kind, half).start()

        def relay(arr_id, half):
            got(arr_id, K_OWN_X, half)
            if half == 0:
                copy(arr_id, K_DIAG, 0).start()
            copy(arr_id, K_FWD_X, half).start()
            got(arr_id, K_OWN_Y, half)
            if half == 1:
                copy(arr_id, K_DIAG, 1).start()
            copy(arr_id, K_FWD_Y, half).start()

        def diag(arr_id, half):
            got(arr_id, K_DIAG, half)
            copy(arr_id, K_FWD_D, half).start()

        def g_copy(mask, incoming=False):
            idx = flip(ex, mask) if incoming else ex
            return pltpu.make_async_remote_copy(
                src_ref=gall.at[idx], dst_ref=gall.at[idx], send_sem=g_send.at[mask - 1], recv_sem=g_recv.at[mask - 1],
                device_id=(st, flip(ex, mask)), device_id_type=MESH)

        own(1, 0)
        own(1, 1)
        load = pltpu.make_async_copy(dy_ref, own_buf, loc_sem.at[0])
        load.start()
        load.wait()
        mine = dyall.at[pl.ds(pl.multiple_of(ex * tok, tok), tok)]
        save = pltpu.make_async_copy(own_buf, mine, loc_sem.at[1])
        save.start()
        pltpu.make_async_remote_copy(
            src_ref=gall.at[ex], dst_ref=gall.at[ex], send_sem=z_send.at[2], recv_sem=z_recv.at[2],
            device_id=(st - n_half, ex), device_id_type=MESH).wait_recv()
        for mask in range(1, 8):
            g_copy(mask).start()

        def x_arrived(half):
            blk = block(xall, 0, half)
            pltpu.make_async_remote_copy(
                src_ref=blk, dst_ref=blk, send_sem=z_send.at[half], recv_sem=z_recv.at[half],
                device_id=(st - n_half, ex), device_id_type=MESH).wait_recv()

        relay(1, 0)
        x_arrived(0)
        own(0, 0)
        relay(1, 1)
        diag(1, 0)
        diag(1, 1)
        relay(0, 0)
        x_arrived(1)
        own(0, 1)
        diag(0, 0)
        relay(0, 1)
        diag(0, 1)
        for arr_id in range(2):
            for half in range(2):
                for kind in (K_OWN_P, K_FWD_X, K_FWD_Y, K_FWD_D):
                    got(arr_id, kind, half)
        for mask in range(1, 8):
            g_copy(mask, incoming=True).wait_recv()
        for arr_id in range(2):
            for half in range(2):
                for kind in range(7):
                    copy(arr_id, kind, half).wait_send()
        for mask in range(1, 8):
            g_copy(mask).wait_send()
        save.wait()


def main_kernel(n_half, xall, dyall, gcol, w1, w3, w2, y_out, dx_out, dw1, dw3, dw2, hbuf, dabuf, dbbuf, sbuf, rbuf,
                w1v, w3v, w2v, xv, dyv, gv, acc, prv, hv, dav, dbv, tv, a1, a3, a2, o1, o3, o2, ov,
                w_sem, in_sem, st_sem, acc_sem, pr_sem, send_sem, recv_sem, t_sem, o_sem, dx_send, dx_recv, y_sem):
    st = lax.axis_index("stage")
    ex = lax.axis_index("expert")
    n_loc, d_model, d_ff = w1v.shape
    tile = xv.shape[1]
    tok = 2 * tile
    n_tiles = xall.shape[0] // tile
    bar = pltpu.get_barrier_semaphore()

    def dx_copy(half):
        return pltpu.make_async_remote_copy(
            src_ref=ov.at[half], dst_ref=dx_out.at[pl.ds(half * tile, tile)], send_sem=dx_send.at[half], recv_sem=dx_recv.at[half],
            device_id=(st - n_half, ex), device_id_type=MESH)

    @pl.when(st < n_half)
    def _():
        pl.semaphore_signal(bar, inc=1, device_id=(st + n_half, ex), device_id_type=MESH)
        pl.semaphore_wait(bar, 1)
        for half in range(2):
            view = dx_out.at[pl.ds(half * tile, tile)]
            pltpu.make_async_remote_copy(
                src_ref=view, dst_ref=view, send_sem=dx_send.at[half], recv_sem=dx_recv.at[half],
                device_id=(st + n_half, ex), device_id_type=MESH).wait_recv()

    @pl.when(st >= n_half)
    def _():
        pl.semaphore_signal(bar, inc=1, device_id=(st - n_half, ex), device_id_type=MESH)
        for mask in (1, 2, 4, 6):
            pl.semaphore_signal(bar, inc=1, device_id=(st, flip(ex, mask)), device_id_type=MESH)
        pl.semaphore_wait(bar, 5)

        w_loads = [pltpu.make_async_copy(a, b, w_sem.at[i]) for i, (a, b) in enumerate(((w1, w1v), (w3, w3v), (w2, w2v)))]
        for c in w_loads:
            c.start()

        def mask_of(k):
            return 7 - k // 2

        def row_of(k):
            return pl.multiple_of(flip(ex, mask_of(k)) * tok + (k % 2) * tile, tile)

        def x_loads(row, slot):
            rows = pl.ds(row, tile)
            return [pltpu.make_async_copy(xall.at[rows], xv.at[slot], in_sem.at[slot, 0]),
                    pltpu.make_async_copy(dyall.at[rows], dyv.at[slot], in_sem.at[slot, 1]),
                    pltpu.make_async_copy(gcol.at[rows], gv.at[slot], in_sem.at[slot, 2])]

        def gate_of(slot, e):
            g = gv[slot]
            lane = lax.broadcasted_iota(jnp.int32, g.shape, 1)
            return jnp.sum(jnp.where(lane == e, g, 0.0), axis=1, keepdims=True)

        def stores(row, e, slot):
            rows = pl.ds(row, tile)
            return [pltpu.make_async_copy(hv.at[slot], hbuf.at[e, rows], st_sem.at[slot, 0]),
                    pltpu.make_async_copy(dav.at[slot], dabuf.at[e, rows], st_sem.at[slot, 1]),
                    pltpu.make_async_copy(dbv.at[slot], dbbuf.at[e, rows], st_sem.at[slot, 2])]

        def slot_no(k):
            mask = mask_of(k)
            half = k % 2
            return jnp.where(mask % 2 == 1, (mask // 2) * 2 + half, 6 + (mask // 2) * 2 + half)

        def rs_copy(p, k):
            mask = mask_of(k)
            slot = slot_no(k)
            target = flip(ex, jnp.where(mask % 2 == 1, 1, mask))
            return pltpu.make_async_remote_copy(
                src_ref=sbuf.at[p, k], dst_ref=rbuf.at[p, slot], send_sem=send_sem.at[p, slot], recv_sem=recv_sem.at[p, slot],
                device_id=(st, target), device_id_type=MESH)

        def rs_arrived(p, slot):
            view = rbuf.at[p, slot]
            pltpu.make_async_remote_copy(
                src_ref=view, dst_ref=view, send_sem=send_sem.at[p, slot], recv_sem=recv_sem.at[p, slot],
                device_id=(st, flip(ex, 1)), device_id_type=MESH).wait_recv()

        def add_arrived(p, slot, dst):
            rs_arrived(p, slot)
            c = pltpu.make_async_copy(rbuf.at[p, slot], prv, pr_sem)
            c.start()
            c.wait()

            def add(i, _):
                rows = pl.ds(pl.multiple_of(i * 64, 64), 64)
                acc[dst, rows] = acc[dst, rows] + prv[rows]
                return 0
            lax.fori_loop(0, tile // 64, add, 0)

        def acc_save(p, k):
            return pltpu.make_async_copy(acc.at[k % 2], sbuf.at[p, k], acc_sem.at[k % 2])

        def finish_step(p, k):
            @pl.when(mask_of(k) % 2 == 0)
            def _():
                add_arrived(p, (mask_of(k) // 2) * 2 + k % 2, k % 2)
            acc_save(p, k).start()

        def send_previous(p, k):
            @pl.when(k > 0)
            def _():
                acc_save(p, k - 1).wait()

                @pl.when(mask_of(k - 1) > 0)
                def _():
                    rs_copy(p, k - 1).start()

        def finalize(p):
            for half in range(2):
                c = pltpu.make_async_copy(sbuf.at[p, 14 + half], acc.at[0], acc_sem.at[0])
                c.start()
                c.wait()
                for mask in (6, 4, 2):
                    add_arrived(p, 6 + mask + half, 0)
                ov[half] = acc[0].astype(BF16)

        for c in x_loads(row_of(0), 0):
            c.start()
        for c in w_loads:
            c.wait()

        def step_one(k, _):
            slot = k % 2
            row = row_of(k)

            @pl.when(k + 1 < n_tiles)
            def _():
                for c in x_loads(row_of(k + 1), (k + 1) % 2):
                    c.start()
            send_previous(0, k)
            for c in x_loads(row, slot):
                c.wait()
            acc[slot] = jnp.zeros(acc.shape[1:], F32)

            def expert(e, _):
                it = k * n_loc + e
                buf = it % 2

                @pl.when(it >= 2)
                def _():
                    for c in stores(row, e, buf):
                        c.wait()
                x = xv[slot]
                g = gate_of(slot, e)
                held = g > 0.0
                pre_gate = jnp.where(held, dot(x, w1v[e], 1, 0), 0.0)
                pre_up = jnp.where(held, dot(x, w3v[e], 1, 0), 0.0)
                sig = jax.nn.sigmoid(pre_gate)
                act = pre_gate * sig
                hv[buf] = (act * pre_up).astype(BF16)
                q = (g * dyv[slot].astype(F32)).astype(BF16)
                dh = dot(q, w2v[e], 1, 1)
                da = (dh * pre_up * sig * (1.0 + pre_gate * (1.0 - sig))).astype(BF16)
                db = (dh * act).astype(BF16)
                dav[buf] = da
                dbv[buf] = db
                c_rows = (dot(da, w1v[e], 1, 1) + dot(db, w3v[e], 1, 1)).astype(BF16)
                acc[slot] = acc[slot] + c_rows.astype(F32)
                for c in stores(row, e, buf):
                    c.start()
                return 0
            lax.fori_loop(0, n_loc, expert, 0)
            finish_step(0, k)
            return 0
        lax.fori_loop(0, n_tiles, step_one, 0)
        acc_save(0, n_tiles - 1).wait()
        for buf in range(2):
            for c in stores(0, 0, buf):
                c.wait()

        def h_loads(k):
            rows = pl.ds(row_of(k), tile)
            return [pltpu.make_async_copy(hbuf.at[e, rows], tv.at[k % 2, e], t_sem.at[k % 2, e]) for e in range(n_loc)] + [
                pltpu.make_async_copy(gcol.at[rows], gv.at[k % 2], in_sem.at[k % 2, 2])]

        for c in h_loads(0):
            c.start()

        def step_two(k, _):
            slot = k % 2

            @pl.when(k + 1 < n_tiles)
            def _():
                for c in h_loads(k + 1):
                    c.start()
            send_previous(1, k)
            for c in h_loads(k):
                c.wait()
            acc[slot] = jnp.zeros(acc.shape[1:], F32)

            def expert(e, _):
                out = dot(tv[slot, e], w2v[e], 1, 0).astype(BF16)
                acc[slot] = acc[slot] + gate_of(slot, e) * out.astype(F32)
                return 0
            lax.fori_loop(0, n_loc, expert, 0)
            finish_step(1, k)
            return 0
        lax.fori_loop(0, n_tiles, step_two, 0)
        acc_save(1, n_tiles - 1).wait()

        def d_loads(it):
            e = it // n_tiles
            slot = it % 2
            row = pl.multiple_of((it % n_tiles) * tile, tile)
            rows = pl.ds(row, tile)
            return x_loads(row, slot) + [
                pltpu.make_async_copy(hbuf.at[e, rows], tv.at[slot, 0], t_sem.at[slot, 0]),
                pltpu.make_async_copy(dabuf.at[e, rows], tv.at[slot, 1], t_sem.at[slot, 1]),
                pltpu.make_async_copy(dbbuf.at[e, rows], tv.at[slot, 2], t_sem.at[slot, 2])]

        def w_saves(e):
            return [pltpu.make_async_copy(o1, dw1.at[e], o_sem.at[0]), pltpu.make_async_copy(o3, dw3.at[e], o_sem.at[1]),
                    pltpu.make_async_copy(o2, dw2.at[e], o_sem.at[2])]

        for c in d_loads(0):
            c.start()
        total = n_loc * n_tiles

        def step_three(it, _):
            e = it // n_tiles
            slot = it % 2

            @pl.when(it + 1 < total)
            def _():
                for c in d_loads(it + 1):
                    c.start()

            @pl.when(it == n_tiles)
            def _():
                finalize(0)
                for half in range(2):
                    dx_copy(half).start()
            for c in d_loads(it):
                c.wait()

            @pl.when(it % n_tiles == 0)
            def _():
                a1[...] = jnp.zeros(a1.shape, F32)
                a3[...] = jnp.zeros(a3.shape, F32)
                a2[...] = jnp.zeros(a2.shape, F32)
            x = xv[slot]
            q = (gate_of(slot, e) * dyv[slot].astype(F32)).astype(BF16)
            a1[...] += dot(x, tv[slot, 1], 0, 0)
            a3[...] += dot(x, tv[slot, 2], 0, 0)
            a2[...] += dot(tv[slot, 0], q, 0, 0)

            @pl.when(it % n_tiles == n_tiles - 1)
            def _():
                @pl.when(e > 0)
                def _():
                    for c in w_saves(e):
                        c.wait()
                o1[...] = a1[...].astype(BF16)
                o3[...] = a3[...].astype(BF16)
                o2[...] = a2[...].astype(BF16)
                for c in w_saves(e):
                    c.start()
            return 0
        lax.fori_loop(0, total, step_three, 0)

        for half in range(2):
            dx_copy(half).wait_send()
        finalize(1)
        for half in range(2):
            c = pltpu.make_async_copy(ov.at[half], y_out.at[pl.ds(half * tile, tile)], y_sem.at[half])
            c.start()
        for half in range(2):
            pltpu.make_async_copy(ov.at[half], y_out.at[pl.ds(half * tile, tile)], y_sem.at[half]).wait()
        for c in w_saves(n_loc - 1):
            c.wait()

        def drain(k, _):
            rs_copy(0, k).wait_send()
            rs_copy(1, k).wait_send()
            return 0
        lax.fori_loop(0, n_tiles - 2, drain, 0)


def solution(mesh):
    n_stage = mesh.shape["stage"]
    n_group = mesh.shape["expert"]
    n_half = n_stage // 2
    tok_spec = P("stage", "expert", None)
    w_spec = P("stage", "expert", None, None)

    def device_fn(tokens_in, expert_ids, gate_wts, w_gate, w_up, w_down, grad_out):
        tok, d_model = tokens_in.shape[1:]
        n_loc, _, d_ff = w_gate.shape[1:]
        n_exp = n_loc * n_group
        lane = tok * n_group
        tile = tok // 2
        n_tiles = lane // tile
        is_b = lax.axis_index("stage") >= n_half
        ex = lax.axis_index("expert")
        ids = expert_ids[0].T[None]
        gate_t = jnp.sum(jnp.where(ids == jnp.arange(n_exp, dtype=jnp.int32)[:, None, None], gate_wts[0].T[None], 0.0), axis=1)

        sds = jax.ShapeDtypeStruct
        dma = pltpu.SemaphoreType.DMA
        xall, dyall, gall = pl.pallas_call(
            functools.partial(gather_kernel, n_half),
            out_shape=(sds((lane, d_model), BF16), sds((lane, d_model), BF16), sds((n_group, n_exp, tok), F32)),
            in_specs=[ANY] * 3,
            out_specs=(ANY,) * 3,
            scratch_shapes=[pltpu.VMEM((tok, d_model), BF16), dma((28,)), dma((28,)), dma((3,)), dma((3,)), dma((7,)), dma((7,)), dma((2,))],
            compiler_params=pltpu.CompilerParams(collective_id=0, has_side_effects=True),
            name="gather_tokens",
        )(tokens_in[0], grad_out[0], gate_t)
        gcol = lax.dynamic_slice_in_dim(gall, ex * n_loc, n_loc, axis=1).transpose(0, 2, 1).reshape(lane, n_loc)

        vm = pltpu.VMEM
        outs = pl.pallas_call(
            functools.partial(main_kernel, n_half),
            out_shape=(
                sds((tok, d_model), BF16), sds((tok, d_model), BF16),
                sds((n_loc, d_model, d_ff), BF16), sds((n_loc, d_model, d_ff), BF16), sds((n_loc, d_ff, d_model), BF16),
                sds((n_loc, lane, d_ff), BF16), sds((n_loc, lane, d_ff), BF16), sds((n_loc, lane, d_ff), BF16),
                sds((2, n_tiles, tile, d_model), F32), sds((2, n_tiles - 2, tile, d_model), F32)),
            in_specs=[ANY] * 6,
            out_specs=(ANY,) * 10,
            scratch_shapes=[
                vm((n_loc, d_model, d_ff), BF16), vm((n_loc, d_model, d_ff), BF16), vm((n_loc, d_ff, d_model), BF16),
                vm((2, tile, d_model), BF16), vm((2, tile, d_model), BF16), vm((2, tile, n_loc), F32),
                vm((2, tile, d_model), F32), vm((tile, d_model), F32),
                vm((2, tile, d_ff), BF16), vm((2, tile, d_ff), BF16), vm((2, tile, d_ff), BF16),
                vm((2, n_loc, tile, d_ff), BF16),
                vm((d_model, d_ff), F32), vm((d_model, d_ff), F32), vm((d_ff, d_model), F32),
                vm((d_model, d_ff), BF16), vm((d_model, d_ff), BF16), vm((d_ff, d_model), BF16),
                vm((2, tile, d_model), BF16),
                dma((3,)), dma((2, 3)), dma((2, 3)), dma((2,)), dma, dma((2, n_tiles - 2)), dma((2, n_tiles - 2)),
                dma((2, n_loc)), dma((3,)), dma((2,)), dma((2,)), dma((2,))],
            compiler_params=pltpu.CompilerParams(collective_id=1, has_side_effects=True, vmem_limit_bytes=63 * 1024 * 1024),
            name="experts",
        )(xall, dyall, gcol, w_gate[0], w_up[0], w_down[0])
        y_local, dx_local, grad_wg, grad_wu, grad_wd = outs[:5]
        on_b = [jnp.where(is_b, v, jnp.zeros_like(v))[None] for v in (y_local, grad_wg, grad_wu, grad_wd)]
        dx_local = jnp.where(is_b, jnp.zeros_like(dx_local), dx_local)
        return on_b[0], dx_local[None], on_b[1], on_b[2], on_b[3]

    return jax.shard_map(device_fn, mesh=mesh, in_specs=(tok_spec, tok_spec, tok_spec, w_spec, w_spec, w_spec, tok_spec), out_specs=(tok_spec, tok_spec, w_spec, w_spec, w_spec), check_vma=False)
```

```python
import functools

import jax
import jax.numpy as jnp
from jax import lax
from jax.experimental import pallas as pl
from jax.experimental.pallas import tpu as pltpu
from jax.sharding import PartitionSpec as P

MESH = pl.DeviceIdType.MESH
ANY = pl.BlockSpec(memory_space=pl.ANY)
F32 = jnp.float32
BF16 = jnp.bfloat16


def flip(ex, mask):
    bit_y = (ex // 4 + mask // 4) % 2
    bit_x = (ex // 2 + mask // 2) % 2
    bit_c = (ex + mask) % 2
    return bit_y * 4 + bit_x * 2 + bit_c


def dot(lhs, rhs, lhs_dim, rhs_dim):
    return lax.dot_general(lhs, rhs, (((lhs_dim,), (rhs_dim,)), ((), ())), preferred_element_type=F32)


AG_KINDS = (
    ((0, 1, 1), (0, 1, 1)),
    ((0, 2, 2), (0, 2, 2)),
    ((0, 4, 4), (0, 4, 4)),
    ((2, 1, 3), (2, 1, 3)),
    ((4, 1, 5), (4, 1, 5)),
    ((2, 4, 6), (4, 2, 6)),
    ((6, 1, 7), (6, 1, 7)),
)
K_OWN_P, K_OWN_X, K_OWN_Y, K_FWD_X, K_FWD_Y, K_DIAG, K_FWD_D = range(7)


def gather_kernel(n_half, n_part, x_ref, dy_ref, g_ref, xall, dyall, gall, own_buf, send_sem, recv_sem, z_send, z_recv, g_send, g_recv, loc_sem):
    st = lax.axis_index("stage")
    ex = lax.axis_index("expert")
    tok = x_ref.shape[0]
    rows_half = tok // n_part
    bar = pltpu.get_barrier_semaphore()

    def block(arr, mask, half):
        start = pl.multiple_of(flip(ex, mask) * tok + half * rows_half, rows_half)
        return arr.at[pl.ds(start, rows_half)]

    def z_copy(half):
        return pltpu.make_async_remote_copy(
            src_ref=x_ref.at[pl.ds(half * rows_half, rows_half)], dst_ref=block(xall, 0, half),
            send_sem=z_send.at[half], recv_sem=z_recv.at[half], device_id=(st + n_half, ex), device_id_type=MESH)

    def zg_copy():
        return pltpu.make_async_remote_copy(
            src_ref=g_ref, dst_ref=gall.at[ex], send_sem=z_send.at[n_part], recv_sem=z_recv.at[n_part],
            device_id=(st + n_half, ex), device_id_type=MESH)

    @pl.when(st < n_half)
    def _():
        pl.semaphore_signal(bar, inc=1, device_id=(st + n_half, ex), device_id_type=MESH)
        pl.semaphore_wait(bar, 1)
        copies = [zg_copy()] + [z_copy(part) for part in range(n_part)]
        for c in copies:
            c.start()
        for c in copies:
            c.wait_send()

    @pl.when(st >= n_half)
    def _():
        pl.semaphore_signal(bar, inc=1, device_id=(st - n_half, ex), device_id_type=MESH)
        for mask in range(1, 8):
            pl.semaphore_signal(bar, inc=1, device_id=(st, flip(ex, mask)), device_id_type=MESH)
        pl.semaphore_wait(bar, 8)

        def copy(arr_id, kind, half, incoming=False):
            arr = (xall, dyall)[arr_id]
            sent, target, got = AG_KINDS[kind][half % 2]
            sem = (arr_id * 7 + kind) * n_part + half
            dst = block(arr, got if incoming else sent, half)
            src = dst
            if sent == 0 and arr_id == 1 and not incoming:
                src = dy_ref.at[pl.ds(half * rows_half, rows_half)]
            return pltpu.make_async_remote_copy(
                src_ref=src, dst_ref=dst, send_sem=send_sem.at[sem], recv_sem=recv_sem.at[sem],
                device_id=(st, flip(ex, target)), device_id_type=MESH)

        def got(arr_id, kind, half):
            copy(arr_id, kind, half, incoming=True).wait_recv()

        def own(arr_id, half):
            for kind in (K_OWN_X, K_OWN_Y, K_OWN_P):
                copy(arr_id, kind, half).start()

        def relay(arr_id, half):
            got(arr_id, K_OWN_X, half)
            if half % 2 == 0:
                copy(arr_id, K_DIAG, half).start()
            copy(arr_id, K_FWD_X, half).start()
            got(arr_id, K_OWN_Y, half)
            if half % 2 == 1:
                copy(arr_id, K_DIAG, half).start()
            copy(arr_id, K_FWD_Y, half).start()

        def diag(arr_id, half):
            got(arr_id, K_DIAG, half)
            copy(arr_id, K_FWD_D, half).start()

        def g_copy(mask, incoming=False):
            idx = flip(ex, mask) if incoming else ex
            return pltpu.make_async_remote_copy(
                src_ref=gall.at[idx], dst_ref=gall.at[idx], send_sem=g_send.at[mask - 1], recv_sem=g_recv.at[mask - 1],
                device_id=(st, flip(ex, mask)), device_id_type=MESH)

        for part in range(n_part):
            own(1, part)
        load = pltpu.make_async_copy(dy_ref, own_buf, loc_sem.at[0])
        load.start()
        load.wait()
        mine = dyall.at[pl.ds(pl.multiple_of(ex * tok, tok), tok)]
        save = pltpu.make_async_copy(own_buf, mine, loc_sem.at[1])
        save.start()
        pltpu.make_async_remote_copy(
            src_ref=gall.at[ex], dst_ref=gall.at[ex], send_sem=z_send.at[n_part], recv_sem=z_recv.at[n_part],
            device_id=(st - n_half, ex), device_id_type=MESH).wait_recv()
        for mask in range(1, 8):
            g_copy(mask).start()

        def x_arrived(half):
            blk = block(xall, 0, half)
            pltpu.make_async_remote_copy(
                src_ref=blk, dst_ref=blk, send_sem=z_send.at[half], recv_sem=z_recv.at[half],
                device_id=(st - n_half, ex), device_id_type=MESH).wait_recv()

        def own_x(part):
            x_arrived(part)
            own(0, part)

        plan = ((relay, 1, 0), (relay, 1, 1), (own_x, 0), (relay, 1, 2), (relay, 1, 3), (diag, 1, 0), (diag, 1, 1), (own_x, 1),
                (relay, 0, 0), (diag, 1, 2), (diag, 1, 3), (own_x, 2), (relay, 0, 1), (diag, 0, 0), (own_x, 3), (relay, 0, 2),
                (diag, 0, 1), (relay, 0, 3), (diag, 0, 2), (diag, 0, 3))
        for act, *where in plan:
            act(*where)
        for arr_id in range(2):
            for half in range(n_part):
                for kind in (K_OWN_P, K_FWD_X, K_FWD_Y, K_FWD_D):
                    got(arr_id, kind, half)
        for mask in range(1, 8):
            g_copy(mask, incoming=True).wait_recv()
        for arr_id in range(2):
            for half in range(n_part):
                for kind in range(7):
                    copy(arr_id, kind, half).wait_send()
        for mask in range(1, 8):
            g_copy(mask).wait_send()
        save.wait()


def main_kernel(n_half, cap, xall, dyall, mrow, mcol, w1, w3, w2, y_out, dx_out, dw1, dw3, dw2, xbuf, qbuf, hbuf, dabuf, dbbuf, sbuf, rbuf,
                w1v, w3v, w2v, xv, dyv, rv, cv, acc, prv, call, ptv, xs, qs, hs, tv, a1, a3, a2,
                w_sem, in_sem, st_sem, acc_sem, pr_sem, send_sem, recv_sem, t_sem, o_sem, dx_send, dx_recv, y_sem):
    st = lax.axis_index("stage")
    ex = lax.axis_index("expert")
    n_loc, d_model, d_ff = w1v.shape
    tok = xv.shape[1]
    tile = tok // 2
    n_blk = rv.shape[0]
    bar = pltpu.get_barrier_semaphore()

    def out_rows(half):
        return call.at[pl.ds(half * tile, tile)]

    def dx_copy(half):
        return pltpu.make_async_remote_copy(
            src_ref=out_rows(half), dst_ref=dx_out.at[pl.ds(half * tile, tile)], send_sem=dx_send.at[half], recv_sem=dx_recv.at[half],
            device_id=(st - n_half, ex), device_id_type=MESH)

    @pl.when(st < n_half)
    def _():
        pl.semaphore_signal(bar, inc=1, device_id=(st + n_half, ex), device_id_type=MESH)
        pl.semaphore_wait(bar, 1)
        for half in range(2):
            view = dx_out.at[pl.ds(half * tile, tile)]
            pltpu.make_async_remote_copy(
                src_ref=view, dst_ref=view, send_sem=dx_send.at[half], recv_sem=dx_recv.at[half],
                device_id=(st + n_half, ex), device_id_type=MESH).wait_recv()

    @pl.when(st >= n_half)
    def _():
        pl.semaphore_signal(bar, inc=1, device_id=(st - n_half, ex), device_id_type=MESH)
        for mask in (1, 2, 4):
            pl.semaphore_signal(bar, inc=1, device_id=(st, flip(ex, mask)), device_id_type=MESH)
        pl.semaphore_wait(bar, 4)

        w_loads = [pltpu.make_async_copy(a, b, w_sem.at[i])
                   for i, (a, b) in enumerate(((mrow, rv), (w1, w1v), (w3, w3v), (w2, w2v)))]
        for c in w_loads:
            c.start()

        def block_rows(k):
            return pl.ds(pl.multiple_of(flip(ex, 7 - k) * tok, tok), tok)

        def col_load(k):
            return pltpu.make_async_copy(mcol.at[block_rows(k)], cv.at[k % 2], in_sem.at[k % 2, 2])

        def x_loads(k):
            slot = k % 2
            return [pltpu.make_async_copy(xall.at[block_rows(k)], xv.at[slot], in_sem.at[slot, 0]),
                    pltpu.make_async_copy(dyall.at[block_rows(k)], dyv.at[slot], in_sem.at[slot, 1]), col_load(k)]

        def pick(slot, half, e):
            rank = cv[slot, half * tile:(half + 1) * tile, e:e + 1]
            return jnp.where(rank == lax.broadcasted_iota(jnp.int32, (tile, cap), 1).astype(F32), 1.0, 0.0).astype(BF16)

        def stores(k, e, buf):
            rows = pl.ds(pl.multiple_of(k * cap, cap), cap)
            mine = pl.ds(pl.multiple_of(buf * cap, cap), cap)
            pairs = [(xs.at[mine], xbuf), (qs.at[mine], qbuf)]
            for i, dst in enumerate((hbuf, dabuf, dbbuf)):
                pairs.append((hs.at[pl.ds(pl.multiple_of((buf * 3 + i) * cap, cap), cap)], dst))
            return [pltpu.make_async_copy(src, dst.at[e, rows], st_sem.at[buf, i]) for i, (src, dst) in enumerate(pairs)]

        def rs_copy(p, k, half):
            mask = 7 - k
            odd = mask % 2 == 1
            slot = jnp.where(odd, (mask // 2) * 2, 6 + mask) + half
            hop = jnp.where(odd, 1, jnp.where(mask == 6, 4 if half else 2, mask))
            return pltpu.make_async_remote_copy(
                src_ref=sbuf.at[p, k, half], dst_ref=rbuf.at[p, slot], send_sem=send_sem.at[p, slot], recv_sem=recv_sem.at[p, slot],
                device_id=(st, flip(ex, hop)), device_id_type=MESH)

        def add_arrived(p, slot, dst):
            view = rbuf.at[p, slot]
            pltpu.make_async_remote_copy(
                src_ref=view, dst_ref=view, send_sem=send_sem.at[p, slot], recv_sem=recv_sem.at[p, slot],
                device_id=(st, flip(ex, 1)), device_id_type=MESH).wait_recv()
            c = pltpu.make_async_copy(view, prv, pr_sem)
            c.start()
            c.wait()

            def add(i, _):
                rows = pl.ds(pl.multiple_of(i * 64, 64), 64)
                acc[dst, rows] = acc[dst, rows] + prv[rows]
                return 0
            lax.fori_loop(0, tile // 64, add, 0)

        def acc_save(p, k, half):
            return pltpu.make_async_copy(acc.at[half], sbuf.at[p, k, half], acc_sem.at[half])

        def finish(p, k, half):
            mask = 7 - k

            @pl.when(mask % 2 == 0)
            def _():
                add_arrived(p, (mask // 2) * 2 + half, half)
            if p == 0:
                @pl.when(mask == (2 if half else 4))
                def _():
                    add_arrived(p, 12 + half, half)
            acc_save(p, k, half).start()

        def send_previous(p, k):
            @pl.when(k > 0)
            def _():
                for half in range(2):
                    acc_save(p, k - 1, half).wait()
                    ready = k < n_blk if p == 0 else k != (6 if half else 4)

                    @pl.when(ready)
                    def _():
                        rs_copy(p, k - 1, half).start()

        def merge(half):
            k = 7 - (2 if half else 4)
            c = pltpu.make_async_copy(sbuf.at[1, k, half], acc.at[half], acc_sem.at[half])
            c.start()
            c.wait()
            add_arrived(1, 12 + half, half)
            acc_save(1, k, half).start()
            acc_save(1, k, half).wait()
            rs_copy(1, k, half).start()

        def finalize(p):
            for half in range(2):
                c = pltpu.make_async_copy(sbuf.at[p, 7, half], acc.at[half], acc_sem.at[half])
                c.start()
                c.wait()
                for mask in (4, 2):
                    add_arrived(p, 6 + mask + half, half)
                call[half * tile:(half + 1) * tile, :] = acc[half].astype(BF16)

        for c in x_loads(0):
            c.start()
        for c in w_loads:
            c.wait()

        def step_one(k, _):
            slot = k % 2
            blk = flip(ex, 7 - k)

            @pl.when(k + 1 < n_blk)
            def _():
                for c in x_loads(k + 1):
                    c.start()
            send_previous(0, k)
            for c in x_loads(k):
                c.wait()

            def expert(e, _):
                it = k * n_loc + e
                buf = it % 2

                @pl.when(it >= 2)
                def _():
                    for c in stores(k, e, buf):
                        c.wait()
                rank = rv[blk, pl.ds(e, 1), :]
                gate = rv[blk, pl.ds(e + n_loc, 1), :]
                held = rank == lax.broadcasted_iota(jnp.int32, (cap, tok), 0).astype(F32)
                take = jnp.where(held, 1.0, 0.0).astype(BF16)
                g = jnp.sum(jnp.where(held, gate, 0.0), axis=1, keepdims=True)
                x = dot(take, xv[slot], 1, 0).astype(BF16)
                q = (g * dot(take, dyv[slot], 1, 0)).astype(BF16)
                pre_gate = dot(x, w1v[e], 1, 0)
                pre_up = dot(x, w3v[e], 1, 0)
                dh = dot(q, w2v[e], 1, 1)
                sig = jax.nn.sigmoid(pre_gate)
                act = pre_gate * sig
                da = (dh * pre_up * sig * (1.0 + pre_gate * (1.0 - sig))).astype(BF16)
                db = (dh * act).astype(BF16)
                mine = pl.ds(pl.multiple_of(buf * cap, cap), cap)
                xs[mine, :] = x
                qs[mine, :] = q
                for i, val in enumerate(((act * pre_up).astype(BF16), da, db)):
                    hs[pl.ds(pl.multiple_of((buf * 3 + i) * cap, cap), cap), :] = val
                call[pl.ds(pl.multiple_of(e * cap, cap), cap), :] = (dot(da, w1v[e], 1, 1) + dot(db, w3v[e], 1, 1)).astype(BF16)
                for c in stores(k, e, buf):
                    c.start()
                return 0
            lax.fori_loop(0, n_loc, expert, 0)
            for half in range(2):
                for e in range(n_loc):
                    ptv[:, e * cap:(e + 1) * cap] = pick(slot, half, e)
                acc[half] = dot(ptv[...], call[...], 1, 0)
                finish(0, k, half)
            return 0
        lax.fori_loop(0, n_blk, step_one, 0)
        for half in range(2):
            acc_save(0, n_blk - 1, half).wait()
        for buf in range(2):
            for c in stores(0, 0, buf):
                c.wait()

        def h_loads(k):
            rows = pl.ds(pl.multiple_of(k * cap, cap), cap)
            return [pltpu.make_async_copy(hbuf.at[e, rows], tv.at[k % 2, pl.ds(e * cap, cap)], t_sem.at[k % 2, e])
                    for e in range(n_loc)] + [col_load(k)]

        for c in h_loads(0):
            c.start()

        def step_two(k, _):
            slot = k % 2

            @pl.when(k + 1 < n_blk)
            def _():
                for c in h_loads(k + 1):
                    c.start()
            send_previous(1, k)
            for c in h_loads(k):
                c.wait()
            for e in range(n_loc):
                out = dot(tv[slot, e * cap:(e + 1) * cap, :], w2v[e], 1, 0).astype(BF16)
                for half in range(2):
                    gate = cv[slot, half * tile:(half + 1) * tile, n_loc + e:n_loc + e + 1]
                    part = gate * dot(pick(slot, half, e), out, 1, 0)
                    acc[half] = part if e == 0 else acc[half] + part
            for half in range(2):
                finish(1, k, half)
            return 0
        lax.fori_loop(0, n_blk, step_two, 0)
        for half in range(2):
            acc_save(1, n_blk - 1, half).wait()

        depth = 2 * cap
        per_e = n_blk // 2

        def d_loads(it):
            e = it // per_e
            slot = it % 2
            rows = pl.ds(pl.multiple_of((it % per_e) * depth, depth), depth)
            top = pl.ds(0, depth)
            return [pltpu.make_async_copy(xbuf.at[e, rows], xv.at[slot, top], in_sem.at[slot, 0]),
                    pltpu.make_async_copy(qbuf.at[e, rows], dyv.at[slot, top], in_sem.at[slot, 1])] + [
                pltpu.make_async_copy(src.at[e, rows], tv.at[slot, pl.ds(i * depth, depth)], t_sem.at[slot, i])
                for i, src in enumerate((hbuf, dabuf, dbbuf))]

        def w_saves(e):
            return [pltpu.make_async_copy(hs.at[pl.ds(0, d_model)], dw1.at[e], o_sem.at[0]),
                    pltpu.make_async_copy(hs.at[pl.ds(d_model, d_model)], dw3.at[e], o_sem.at[1]),
                    pltpu.make_async_copy(qs.at[pl.ds(0, d_ff)], dw2.at[e], o_sem.at[2])]

        for c in d_loads(0):
            c.start()
        total = n_loc * per_e

        def step_three(it, _):
            e = it // per_e
            slot = it % 2

            @pl.when(it + 1 < total)
            def _():
                for c in d_loads(it + 1):
                    c.start()

            @pl.when(it == 2)
            def _():
                finalize(0)
                for half in range(2):
                    dx_copy(half).start()

            @pl.when(it == 8)
            def _():
                merge(1)

            @pl.when(it == 12)
            def _():
                merge(0)
            for c in d_loads(it):
                c.wait()

            @pl.when(it % per_e == 0)
            def _():
                a1[...] = jnp.zeros(a1.shape, F32)
                a3[...] = jnp.zeros(a3.shape, F32)
                a2[...] = jnp.zeros(a2.shape, F32)
            x = xv[slot, 0:depth, :]
            a1[...] += dot(x, tv[slot, depth:2 * depth, :], 0, 0)
            a3[...] += dot(x, tv[slot, 2 * depth:3 * depth, :], 0, 0)
            a2[...] += dot(tv[slot, 0:depth, :], dyv[slot, 0:depth, :], 0, 0)

            @pl.when(it % per_e == per_e - 1)
            def _():
                @pl.when(e > 0)
                def _():
                    for c in w_saves(e):
                        c.wait()
                hs[0:d_model, :] = a1[...].astype(BF16)
                hs[d_model:2 * d_model, :] = a3[...].astype(BF16)
                qs[0:d_ff, :] = a2[...].astype(BF16)
                for c in w_saves(e):
                    c.start()
            return 0
        lax.fori_loop(0, total, step_three, 0)

        for half in range(2):
            dx_copy(half).wait_send()
        finalize(1)

        def y_save(half):
            return pltpu.make_async_copy(out_rows(half), y_out.at[pl.ds(half * tile, tile)], y_sem.at[half])
        for half in range(2):
            y_save(half).start()
        for half in range(2):
            y_save(half).wait()
        for c in w_saves(n_loc - 1):
            c.wait()

        def drain(k, _):
            for p in range(2):
                for half in range(2):
                    rs_copy(p, k, half).wait_send()
            return 0
        lax.fori_loop(0, n_blk - 1, drain, 0)


def solution(mesh):
    n_stage = mesh.shape["stage"]
    n_group = mesh.shape["expert"]
    n_half = n_stage // 2
    tok_spec = P("stage", "expert", None)
    w_spec = P("stage", "expert", None, None)

    def device_fn(tokens_in, expert_ids, gate_wts, w_gate, w_up, w_down, grad_out):
        tok, d_model = tokens_in.shape[1:]
        n_loc, _, d_ff = w_gate.shape[1:]
        n_exp = n_loc * n_group
        lane = tok * n_group
        tile = tok // 2
        top_k = expert_ids.shape[2]
        cap = 3 * tok * top_k // (2 * n_exp)
        n_part = 4
        is_b = lax.axis_index("stage") >= n_half
        ex = lax.axis_index("expert")
        ids = expert_ids[0].T[None]
        gate_t = jnp.sum(jnp.where(ids == jnp.arange(n_exp, dtype=jnp.int32)[:, None, None], gate_wts[0].T[None], 0.0), axis=1)

        sds = jax.ShapeDtypeStruct
        dma = pltpu.SemaphoreType.DMA
        xall, dyall, gall = pl.pallas_call(
            functools.partial(gather_kernel, n_half, n_part),
            out_shape=(sds((lane, d_model), BF16), sds((lane, d_model), BF16), sds((n_group, n_exp, tok), F32)),
            in_specs=[ANY] * 3,
            out_specs=(ANY,) * 3,
            scratch_shapes=[pltpu.VMEM((tok, d_model), BF16), dma((14 * n_part,)), dma((14 * n_part,)), dma((n_part + 1,)), dma((n_part + 1,)), dma((7,)), dma((7,)), dma((2,))],
            compiler_params=pltpu.CompilerParams(collective_id=0, has_side_effects=True),
            name="gather_tokens",
        )(tokens_in[0], grad_out[0], gate_t)
        gate_row = lax.dynamic_slice_in_dim(gall, ex * n_loc, n_loc, axis=1)
        held = gate_row > 0.0
        upper = (jnp.arange(tok)[:, None] <= jnp.arange(tok)[None, :]).astype(BF16)
        count = jnp.einsum("set,tu->seu", held.astype(BF16), upper, preferred_element_type=F32)
        mrow = jnp.concatenate([jnp.where(held, count - 1.0, -1.0), gate_row], axis=1)
        mcol = mrow.transpose(0, 2, 1).reshape(lane, 2 * n_loc)

        vm = pltpu.VMEM
        rows = n_group * cap
        outs = pl.pallas_call(
            functools.partial(main_kernel, n_half, cap),
            out_shape=(
                sds((tok, d_model), BF16), sds((tok, d_model), BF16),
                sds((n_loc, d_model, d_ff), BF16), sds((n_loc, d_model, d_ff), BF16), sds((n_loc, d_ff, d_model), BF16),
                sds((n_loc, rows, d_model), BF16), sds((n_loc, rows, d_model), BF16),
                sds((n_loc, rows, d_ff), BF16), sds((n_loc, rows, d_ff), BF16), sds((n_loc, rows, d_ff), BF16),
                sds((2, n_group, 2, tile, d_model), F32), sds((2, 14, tile, d_model), F32)),
            in_specs=[ANY] * 7,
            out_specs=(ANY,) * 12,
            scratch_shapes=[
                vm((n_loc, d_model, d_ff), BF16), vm((n_loc, d_model, d_ff), BF16), vm((n_loc, d_ff, d_model), BF16),
                vm((2, tok, d_model), BF16), vm((2, tok, d_model), BF16), vm((n_group, 2 * n_loc, tok), F32), vm((2, tok, 2 * n_loc), F32),
                vm((2, tile, d_model), F32), vm((tile, d_model), F32), vm((n_loc * cap, d_model), BF16), vm((tile, n_loc * cap), BF16),
                vm((2 * cap, d_model), BF16), vm((2 * cap, d_model), BF16), vm((6 * cap, d_ff), BF16), vm((2, 6 * cap, d_ff), BF16),
                vm((d_model, d_ff), F32), vm((d_model, d_ff), F32), vm((d_ff, d_model), F32),
                dma((4,)), dma((2, 3)), dma((2, 5)), dma((2,)), dma, dma((2, 14)), dma((2, 14)),
                dma((2, n_loc)), dma((3,)), dma((2,)), dma((2,)), dma((2,))],
            compiler_params=pltpu.CompilerParams(collective_id=1, has_side_effects=True, vmem_limit_bytes=63 * 1024 * 1024),
            name="experts",
        )(xall, dyall, mrow, mcol, w_gate[0], w_up[0], w_down[0])
        y_local, dx_local, grad_wg, grad_wu, grad_wd = outs[:5]
        on_b = [jnp.where(is_b, v, jnp.zeros_like(v))[None] for v in (y_local, grad_wg, grad_wu, grad_wd)]
        dx_local = jnp.where(is_b, jnp.zeros_like(dx_local), dx_local)
        return on_b[0], dx_local[None], on_b[1], on_b[2], on_b[3]

    return jax.shard_map(device_fn, mesh=mesh, in_specs=(tok_spec, tok_spec, tok_spec, w_spec, w_spec, w_spec, tok_spec), out_specs=(tok_spec, tok_spec, w_spec, w_spec, w_spec), check_vma=False)
```

```python
import functools

import jax
import jax.numpy as jnp
from jax import lax
from jax.experimental import pallas as pl
from jax.experimental.pallas import tpu as pltpu
from jax.sharding import PartitionSpec as P

MESH = pl.DeviceIdType.MESH
ANY = pl.BlockSpec(memory_space=pl.ANY)
F32 = jnp.float32
BF16 = jnp.bfloat16


def flip(ex, mask):
    bit_y = (ex // 4 + mask // 4) % 2
    bit_x = (ex // 2 + mask // 2) % 2
    bit_c = (ex + mask) % 2
    return bit_y * 4 + bit_x * 2 + bit_c


def dot(lhs, rhs, lhs_dim, rhs_dim):
    return lax.dot_general(lhs, rhs, (((lhs_dim,), (rhs_dim,)), ((), ())), preferred_element_type=F32)


AG_KINDS = (
    ((0, 1, 1), (0, 1, 1)),
    ((0, 2, 2), (0, 2, 2)),
    ((0, 4, 4), (0, 4, 4)),
    ((2, 1, 3), (2, 1, 3)),
    ((4, 1, 5), (4, 1, 5)),
    ((2, 4, 6), (4, 2, 6)),
    ((6, 1, 7), (6, 1, 7)),
)
K_OWN_P, K_OWN_X, K_OWN_Y, K_FWD_X, K_FWD_Y, K_DIAG, K_FWD_D = range(7)


def gather_kernel(n_half, n_part, x_ref, dy_ref, g_ref, xall, dyall, gall, own_buf, send_sem, recv_sem, z_send, z_recv, g_send, g_recv, loc_sem):
    st = lax.axis_index("stage")
    ex = lax.axis_index("expert")
    tok = x_ref.shape[0]
    rows_half = tok // n_part
    bar = pltpu.get_barrier_semaphore()

    def block(arr, mask, half):
        start = pl.multiple_of(flip(ex, mask) * tok + half * rows_half, rows_half)
        return arr.at[pl.ds(start, rows_half)]

    def z_copy(half):
        return pltpu.make_async_remote_copy(
            src_ref=x_ref.at[pl.ds(half * rows_half, rows_half)], dst_ref=block(xall, 0, half),
            send_sem=z_send.at[half], recv_sem=z_recv.at[half], device_id=(st + n_half, ex), device_id_type=MESH)

    def zg_copy():
        return pltpu.make_async_remote_copy(
            src_ref=g_ref, dst_ref=gall.at[ex], send_sem=z_send.at[n_part], recv_sem=z_recv.at[n_part],
            device_id=(st + n_half, ex), device_id_type=MESH)

    @pl.when(st < n_half)
    def _():
        pl.semaphore_signal(bar, inc=1, device_id=(st + n_half, ex), device_id_type=MESH)
        pl.semaphore_wait(bar, 1)
        copies = [zg_copy()] + [z_copy(part) for part in range(n_part)]
        for c in copies:
            c.start()
        for c in copies:
            c.wait_send()

    @pl.when(st >= n_half)
    def _():
        pl.semaphore_signal(bar, inc=1, device_id=(st - n_half, ex), device_id_type=MESH)
        for mask in range(1, 8):
            pl.semaphore_signal(bar, inc=1, device_id=(st, flip(ex, mask)), device_id_type=MESH)
        pl.semaphore_wait(bar, 8)

        def copy(arr_id, kind, half, incoming=False):
            arr = (xall, dyall)[arr_id]
            sent, target, got = AG_KINDS[kind][half % 2]
            sem = (arr_id * 7 + kind) * n_part + half
            dst = block(arr, got if incoming else sent, half)
            src = dst
            if sent == 0 and arr_id == 1 and not incoming:
                src = dy_ref.at[pl.ds(half * rows_half, rows_half)]
            return pltpu.make_async_remote_copy(
                src_ref=src, dst_ref=dst, send_sem=send_sem.at[sem], recv_sem=recv_sem.at[sem],
                device_id=(st, flip(ex, target)), device_id_type=MESH)

        def got(arr_id, kind, half):
            copy(arr_id, kind, half, incoming=True).wait_recv()

        def own(arr_id, half):
            for kind in (K_OWN_X, K_OWN_Y, K_OWN_P):
                copy(arr_id, kind, half).start()

        def relay(arr_id, half):
            got(arr_id, K_OWN_X, half)
            if half % 2 == 0:
                copy(arr_id, K_DIAG, half).start()
            copy(arr_id, K_FWD_X, half).start()
            got(arr_id, K_OWN_Y, half)
            if half % 2 == 1:
                copy(arr_id, K_DIAG, half).start()
            copy(arr_id, K_FWD_Y, half).start()

        def diag(arr_id, half):
            got(arr_id, K_DIAG, half)
            copy(arr_id, K_FWD_D, half).start()

        def g_copy(mask, incoming=False):
            idx = flip(ex, mask) if incoming else ex
            return pltpu.make_async_remote_copy(
                src_ref=gall.at[idx], dst_ref=gall.at[idx], send_sem=g_send.at[mask - 1], recv_sem=g_recv.at[mask - 1],
                device_id=(st, flip(ex, mask)), device_id_type=MESH)

        for part in range(n_part):
            own(1, part)
        load = pltpu.make_async_copy(dy_ref, own_buf, loc_sem.at[0])
        load.start()
        load.wait()
        mine = dyall.at[pl.ds(pl.multiple_of(ex * tok, tok), tok)]
        save = pltpu.make_async_copy(own_buf, mine, loc_sem.at[1])
        save.start()
        pltpu.make_async_remote_copy(
            src_ref=gall.at[ex], dst_ref=gall.at[ex], send_sem=z_send.at[n_part], recv_sem=z_recv.at[n_part],
            device_id=(st - n_half, ex), device_id_type=MESH).wait_recv()
        for mask in range(1, 8):
            g_copy(mask).start()

        def x_arrived(half):
            blk = block(xall, 0, half)
            pltpu.make_async_remote_copy(
                src_ref=blk, dst_ref=blk, send_sem=z_send.at[half], recv_sem=z_recv.at[half],
                device_id=(st - n_half, ex), device_id_type=MESH).wait_recv()

        def own_x(part):
            x_arrived(part)
            own(0, part)

        plan = []
        for part in range(n_part):
            at = (part + 1) / n_part
            x_at = max(100 * at, 67) + 15
            plan += [(45 * at, relay, 1, part), (50 + 22 * at, diag, 1, part), (100 * at, own_x, part),
                     (x_at, relay, 0, part), (x_at + 12, diag, 0, part)]
        plan = [item[1:] for item in sorted(plan, key=lambda item: item[0])]
        for act, *where in plan:
            act(*where)
        for arr_id in range(2):
            for half in range(n_part):
                for kind in (K_OWN_P, K_FWD_X, K_FWD_Y, K_FWD_D):
                    got(arr_id, kind, half)
        for mask in range(1, 8):
            g_copy(mask, incoming=True).wait_recv()
        for arr_id in range(2):
            for half in range(n_part):
                for kind in range(7):
                    copy(arr_id, kind, half).wait_send()
        for mask in range(1, 8):
            g_copy(mask).wait_send()
        save.wait()


def main_kernel(n_half, cap, xall, dyall, mrow, mcol, w1, w3, w2, y_out, dx_out, dw1, dw3, dw2, xbuf, qbuf, hbuf, dabuf, dbbuf, sbuf, rbuf,
                w1v, w3v, w2v, xv, dyv, rv, cv, cw, acc, prv, call, ptv, xs, qs, hs, tv, a1, a3, a2,
                w_sem, in_sem, cw_sem, st_sem, acc_sem, pr_sem, send_sem, recv_sem, t_sem, o_sem, dx_send, dx_recv, y_sem):
    st = lax.axis_index("stage")
    ex = lax.axis_index("expert")
    n_loc, d_model, d_ff = w1v.shape
    tok = xv.shape[1]
    tile = tok // 2
    n_blk = rv.shape[0]
    bar = pltpu.get_barrier_semaphore()

    def out_rows(half):
        return call.at[pl.ds(half * tile, tile)]

    def dx_copy(half):
        return pltpu.make_async_remote_copy(
            src_ref=out_rows(half), dst_ref=dx_out.at[pl.ds(half * tile, tile)], send_sem=dx_send.at[half], recv_sem=dx_recv.at[half],
            device_id=(st - n_half, ex), device_id_type=MESH)

    @pl.when(st < n_half)
    def _():
        pl.semaphore_signal(bar, inc=1, device_id=(st + n_half, ex), device_id_type=MESH)
        pl.semaphore_wait(bar, 1)
        for half in range(2):
            view = dx_out.at[pl.ds(half * tile, tile)]
            pltpu.make_async_remote_copy(
                src_ref=view, dst_ref=view, send_sem=dx_send.at[half], recv_sem=dx_recv.at[half],
                device_id=(st + n_half, ex), device_id_type=MESH).wait_recv()

    @pl.when(st >= n_half)
    def _():
        pl.semaphore_signal(bar, inc=1, device_id=(st - n_half, ex), device_id_type=MESH)
        for mask in (1, 2, 4):
            pl.semaphore_signal(bar, inc=1, device_id=(st, flip(ex, mask)), device_id_type=MESH)
        pl.semaphore_wait(bar, 4)

        w_loads = [pltpu.make_async_copy(a, b, w_sem.at[i])
                   for i, (a, b) in enumerate(((mrow, rv), (w1, w1v), (w3, w3v), (w2, w2v)))]
        for c in w_loads:
            c.start()

        def block_rows(k):
            return pl.ds(pl.multiple_of(flip(ex, 7 - k) * tok, tok), tok)

        def col_load(k):
            return pltpu.make_async_copy(mcol.at[block_rows(k)], cv.at[k % 2], in_sem.at[k % 2, 2])

        def x_loads(k):
            slot = k % 2
            return [pltpu.make_async_copy(xall.at[block_rows(k)], xv.at[slot], in_sem.at[slot, 0]),
                    pltpu.make_async_copy(dyall.at[block_rows(k)], dyv.at[slot], in_sem.at[slot, 1]), col_load(k)]

        def pick(meta, slot, half, e):
            rank = meta[slot, half * tile:(half + 1) * tile, e:e + 1]
            return jnp.where(rank == lax.broadcasted_iota(jnp.int32, (tile, cap), 1).astype(F32), 1.0, 0.0).astype(BF16)

        def stores(k, e, buf):
            rows = pl.ds(pl.multiple_of(k * cap, cap), cap)
            mine = pl.ds(pl.multiple_of(buf * cap, cap), cap)
            pairs = [(xs.at[mine], xbuf), (qs.at[mine], qbuf)]
            for i, dst in enumerate((hbuf, dabuf, dbbuf)):
                pairs.append((hs.at[pl.ds(pl.multiple_of((buf * 3 + i) * cap, cap), cap)], dst))
            return [pltpu.make_async_copy(src, dst.at[e, rows], st_sem.at[buf, i]) for i, (src, dst) in enumerate(pairs)]

        def rs_copy(p, k, half):
            mask = 7 - k
            odd = mask % 2 == 1
            slot = jnp.where(odd, (mask // 2) * 2, 6 + mask) + half
            hop = jnp.where(odd, 1, jnp.where(mask == 6, 4 if half else 2, mask))
            return pltpu.make_async_remote_copy(
                src_ref=sbuf.at[p, k, half], dst_ref=rbuf.at[p, slot], send_sem=send_sem.at[p, slot], recv_sem=recv_sem.at[p, slot],
                device_id=(st, flip(ex, hop)), device_id_type=MESH)

        def add_arrived(p, slot, dst):
            view = rbuf.at[p, slot]
            pltpu.make_async_remote_copy(
                src_ref=view, dst_ref=view, send_sem=send_sem.at[p, slot], recv_sem=recv_sem.at[p, slot],
                device_id=(st, flip(ex, 1)), device_id_type=MESH).wait_recv()
            c = pltpu.make_async_copy(view, prv, pr_sem)
            c.start()
            c.wait()

            def add(i, _):
                rows = pl.ds(pl.multiple_of(i * 64, 64), 64)
                acc[dst, rows] = acc[dst, rows] + prv[rows]
                return 0
            lax.fori_loop(0, tile // 64, add, 0)

        def acc_save(p, k, half):
            return pltpu.make_async_copy(acc.at[half], sbuf.at[p, k, half], acc_sem.at[half])

        def finish(p, k, half):
            mask = 7 - k

            @pl.when(mask % 2 == 0)
            def _():
                add_arrived(p, (mask // 2) * 2 + half, half)
            @pl.when(mask == (2 if half else 4))
            def _():
                add_arrived(p, 12 + half, half)
            acc_save(p, k, half).start()

        def send(p, k):
            for half in range(2):
                acc_save(p, k, half).wait()

                @pl.when(k < n_blk - 1)
                def _():
                    rs_copy(p, k, half).start()

        def finalize(p):
            for half in range(2):
                c = pltpu.make_async_copy(sbuf.at[p, 7, half], acc.at[half], acc_sem.at[half])
                c.start()
                c.wait()
                for mask in (4, 2):
                    add_arrived(p, 6 + mask + half, half)
                call[half * tile:(half + 1) * tile, :] = acc[half].astype(BF16)

        for c in x_loads(0):
            c.start()
        for c in w_loads:
            c.wait()

        def step_one(first, k):
            slot = k % 2
            blk = flip(ex, 7 - k)

            @pl.when(k + 1 < n_blk)
            def _():
                for c in x_loads(k + 1):
                    c.start()
            for c in x_loads(k):
                c.wait()

            def expert(e, _):
                it = k * n_loc + e
                buf = it % 2

                @pl.when(it >= first * n_loc + 2)
                def _():
                    for c in stores(k, e, buf):
                        c.wait()
                rank = rv[blk, pl.ds(e, 1), :]
                gate = rv[blk, pl.ds(e + n_loc, 1), :]
                held = rank == lax.broadcasted_iota(jnp.int32, (cap, tok), 0).astype(F32)
                take = jnp.where(held, 1.0, 0.0).astype(BF16)
                g = jnp.sum(jnp.where(held, gate, 0.0), axis=1, keepdims=True)
                x = dot(take, xv[slot], 1, 0).astype(BF16)
                q = (g * dot(take, dyv[slot], 1, 0)).astype(BF16)
                pre_gate = dot(x, w1v[e], 1, 0)
                pre_up = dot(x, w3v[e], 1, 0)
                dh = dot(q, w2v[e], 1, 1)
                sig = jax.nn.sigmoid(pre_gate)
                act = pre_gate * sig
                da = (dh * pre_up * sig * (1.0 + pre_gate * (1.0 - sig))).astype(BF16)
                db = (dh * act).astype(BF16)
                mine = pl.ds(pl.multiple_of(buf * cap, cap), cap)
                xs[mine, :] = x
                qs[mine, :] = q
                for i, val in enumerate(((act * pre_up).astype(BF16), da, db)):
                    hs[pl.ds(pl.multiple_of((buf * 3 + i) * cap, cap), cap), :] = val
                call[pl.ds(pl.multiple_of(e * cap, cap), cap), :] = (dot(da, w1v[e], 1, 1) + dot(db, w3v[e], 1, 1)).astype(BF16)
                for c in stores(k, e, buf):
                    c.start()
                return 0
            lax.fori_loop(0, n_loc, expert, 0)
            for half in range(2):
                for e in range(n_loc):
                    ptv[:, e * cap:(e + 1) * cap] = pick(cv, slot, half, e)
                acc[half] = dot(ptv[...], call[...], 1, 0)
                finish(0, k, half)

        def h_loads(k):
            rows = pl.ds(pl.multiple_of(k * cap, cap), cap)
            return [pltpu.make_async_copy(hbuf.at[e, rows], tv.at[k % 2, pl.ds(e * cap, cap)], t_sem.at[k % 2, e])
                    for e in range(n_loc)] + [pltpu.make_async_copy(mcol.at[block_rows(k)], cw.at[k % 2], cw_sem.at[k % 2])]

        def step_two(last, k):
            slot = k % 2

            @pl.when(k + 1 < last)
            def _():
                for c in h_loads(k + 1):
                    c.start()
            for c in h_loads(k):
                c.wait()
            for e in range(n_loc):
                out = dot(tv[slot, e * cap:(e + 1) * cap, :], w2v[e], 1, 0).astype(BF16)
                for half in range(2):
                    gate = cw[slot, half * tile:(half + 1) * tile, n_loc + e:n_loc + e + 1]
                    part = gate * dot(pick(cw, slot, half, e), out, 1, 0)
                    acc[half] = part if e == 0 else acc[half] + part
            for half in range(2):
                finish(1, k, half)

        last_one = n_blk + 2
        n_steps = 2 * n_blk

        def plan_of(t):
            early = t < 4
            two = jnp.where(early, t // 2, jnp.where(t < last_one, 0, 1))
            k = jnp.where(early, t % 2, jnp.where(t < last_one, t - 2, t - n_blk))
            return two, k

        def step(t, _):
            two, k = plan_of(t)

            @pl.when(t > 0)
            def _():
                send(*plan_of(t - 1))

            @pl.when(two == 0)
            def _():
                step_one(jnp.where(t < 4, 0, 2), k)

            @pl.when((t == 2) | (t == last_one))
            def _():
                for buf in range(2):
                    for c in stores(0, 0, buf):
                        c.wait()
                for c in h_loads(k):
                    c.start()

            @pl.when(two == 1)
            def _():
                step_two(jnp.where(t < 4, 2, n_blk), k)
            return 0
        lax.fori_loop(0, n_steps, step, 0)
        for half in range(2):
            acc_save(1, n_blk - 1, half).wait()

        depth = 2 * cap
        per_e = n_blk // 2

        def d_loads(it):
            e = it // per_e
            slot = it % 2
            rows = pl.ds(pl.multiple_of((it % per_e) * depth, depth), depth)
            top = pl.ds(0, depth)
            return [pltpu.make_async_copy(xbuf.at[e, rows], xv.at[slot, top], in_sem.at[slot, 0]),
                    pltpu.make_async_copy(qbuf.at[e, rows], dyv.at[slot, top], in_sem.at[slot, 1])] + [
                pltpu.make_async_copy(src.at[e, rows], tv.at[slot, pl.ds(i * depth, depth)], t_sem.at[slot, i])
                for i, src in enumerate((hbuf, dabuf, dbbuf))]

        def w_saves(e):
            return [pltpu.make_async_copy(hs.at[pl.ds(0, d_model)], dw1.at[e], o_sem.at[0]),
                    pltpu.make_async_copy(hs.at[pl.ds(d_model, d_model)], dw3.at[e], o_sem.at[1]),
                    pltpu.make_async_copy(qs.at[pl.ds(0, d_ff)], dw2.at[e], o_sem.at[2])]

        for c in d_loads(0):
            c.start()
        total = n_loc * per_e

        def step_three(it, _):
            e = it // per_e
            slot = it % 2

            @pl.when(it + 1 < total)
            def _():
                for c in d_loads(it + 1):
                    c.start()

            @pl.when(it == 1)
            def _():
                finalize(0)
                for half in range(2):
                    dx_copy(half).start()

            for c in d_loads(it):
                c.wait()

            @pl.when(it % per_e == 0)
            def _():
                a1[...] = jnp.zeros(a1.shape, F32)
                a3[...] = jnp.zeros(a3.shape, F32)
                a2[...] = jnp.zeros(a2.shape, F32)
            x = xv[slot, 0:depth, :]
            a1[...] += dot(x, tv[slot, depth:2 * depth, :], 0, 0)
            a3[...] += dot(x, tv[slot, 2 * depth:3 * depth, :], 0, 0)
            a2[...] += dot(tv[slot, 0:depth, :], dyv[slot, 0:depth, :], 0, 0)

            @pl.when(it % per_e == per_e - 1)
            def _():
                @pl.when(e > 0)
                def _():
                    for c in w_saves(e):
                        c.wait()
                hs[0:d_model, :] = a1[...].astype(BF16)
                hs[d_model:2 * d_model, :] = a3[...].astype(BF16)
                qs[0:d_ff, :] = a2[...].astype(BF16)
                for c in w_saves(e):
                    c.start()
            return 0
        lax.fori_loop(0, total, step_three, 0)

        for half in range(2):
            dx_copy(half).wait_send()
        finalize(1)

        def y_save(half):
            return pltpu.make_async_copy(out_rows(half), y_out.at[pl.ds(half * tile, tile)], y_sem.at[half])
        for half in range(2):
            y_save(half).start()
        for half in range(2):
            y_save(half).wait()
        for c in w_saves(n_loc - 1):
            c.wait()

        def drain(k, _):
            for p in range(2):
                for half in range(2):
                    rs_copy(p, k, half).wait_send()
            return 0
        lax.fori_loop(0, n_blk - 1, drain, 0)


def solution(mesh):
    n_stage = mesh.shape["stage"]
    n_group = mesh.shape["expert"]
    n_half = n_stage // 2
    tok_spec = P("stage", "expert", None)
    w_spec = P("stage", "expert", None, None)

    def device_fn(tokens_in, expert_ids, gate_wts, w_gate, w_up, w_down, grad_out):
        tok, d_model = tokens_in.shape[1:]
        n_loc, _, d_ff = w_gate.shape[1:]
        n_exp = n_loc * n_group
        lane = tok * n_group
        tile = tok // 2
        top_k = expert_ids.shape[2]
        cap = 3 * tok * top_k // (2 * n_exp)
        n_part = 4
        is_b = lax.axis_index("stage") >= n_half
        ex = lax.axis_index("expert")
        ids = expert_ids[0].T[None]
        gate_t = jnp.sum(jnp.where(ids == jnp.arange(n_exp, dtype=jnp.int32)[:, None, None], gate_wts[0].T[None], 0.0), axis=1)

        sds = jax.ShapeDtypeStruct
        dma = pltpu.SemaphoreType.DMA
        xall, dyall, gall = pl.pallas_call(
            functools.partial(gather_kernel, n_half, n_part),
            out_shape=(sds((lane, d_model), BF16), sds((lane, d_model), BF16), sds((n_group, n_exp, tok), F32)),
            in_specs=[ANY] * 3,
            out_specs=(ANY,) * 3,
            scratch_shapes=[pltpu.VMEM((tok, d_model), BF16), dma((14 * n_part,)), dma((14 * n_part,)), dma((n_part + 1,)), dma((n_part + 1,)), dma((7,)), dma((7,)), dma((2,))],
            compiler_params=pltpu.CompilerParams(collective_id=0, has_side_effects=True),
            name="gather_tokens",
        )(tokens_in[0], grad_out[0], gate_t)
        gate_row = lax.dynamic_slice_in_dim(gall, ex * n_loc, n_loc, axis=1)
        held = gate_row > 0.0
        upper = (jnp.arange(tok)[:, None] <= jnp.arange(tok)[None, :]).astype(BF16)
        count = jnp.einsum("set,tu->seu", held.astype(BF16), upper, preferred_element_type=F32)
        mrow = jnp.concatenate([jnp.where(held, count - 1.0, -1.0), gate_row], axis=1)
        mcol = mrow.transpose(0, 2, 1).reshape(lane, 2 * n_loc)

        vm = pltpu.VMEM
        rows = n_group * cap
        outs = pl.pallas_call(
            functools.partial(main_kernel, n_half, cap),
            out_shape=(
                sds((tok, d_model), BF16), sds((tok, d_model), BF16),
                sds((n_loc, d_model, d_ff), BF16), sds((n_loc, d_model, d_ff), BF16), sds((n_loc, d_ff, d_model), BF16),
                sds((n_loc, rows, d_model), BF16), sds((n_loc, rows, d_model), BF16),
                sds((n_loc, rows, d_ff), BF16), sds((n_loc, rows, d_ff), BF16), sds((n_loc, rows, d_ff), BF16),
                sds((2, n_group, 2, tile, d_model), F32), sds((2, 14, tile, d_model), F32)),
            in_specs=[ANY] * 7,
            out_specs=(ANY,) * 12,
            scratch_shapes=[
                vm((n_loc, d_model, d_ff), BF16), vm((n_loc, d_model, d_ff), BF16), vm((n_loc, d_ff, d_model), BF16),
                vm((2, tok, d_model), BF16), vm((2, tok, d_model), BF16), vm((n_group, 2 * n_loc, tok), F32), vm((2, tok, 2 * n_loc), F32),
                vm((2, tok, 2 * n_loc), F32),
                vm((2, tile, d_model), F32), vm((tile, d_model), F32), vm((n_loc * cap, d_model), BF16), vm((tile, n_loc * cap), BF16),
                vm((2 * cap, d_model), BF16), vm((2 * cap, d_model), BF16), vm((6 * cap, d_ff), BF16), vm((2, 6 * cap, d_ff), BF16),
                vm((d_model, d_ff), F32), vm((d_model, d_ff), F32), vm((d_ff, d_model), F32),
                dma((4,)), dma((2, 3)), dma((2,)), dma((2, 5)), dma((2,)), dma, dma((2, 14)), dma((2, 14)),
                dma((2, n_loc)), dma((3,)), dma((2,)), dma((2,)), dma((2,))],
            compiler_params=pltpu.CompilerParams(collective_id=1, has_side_effects=True, vmem_limit_bytes=63 * 1024 * 1024),
            name="experts",
        )(xall, dyall, mrow, mcol, w_gate[0], w_up[0], w_down[0])
        y_local, dx_local, grad_wg, grad_wu, grad_wd = outs[:5]
        on_b = [jnp.where(is_b, v, jnp.zeros_like(v))[None] for v in (y_local, grad_wg, grad_wu, grad_wd)]
        dx_local = jnp.where(is_b, jnp.zeros_like(dx_local), dx_local)
        return on_b[0], dx_local[None], on_b[1], on_b[2], on_b[3]

    return jax.shard_map(device_fn, mesh=mesh, in_specs=(tok_spec, tok_spec, tok_spec, w_spec, w_spec, w_spec, tok_spec), out_specs=(tok_spec, tok_spec, w_spec, w_spec, w_spec), check_vma=False)
```

```python
import functools

import jax
import jax.numpy as jnp
from jax import lax
from jax.experimental import pallas as pl
from jax.experimental.pallas import tpu as pltpu
from jax.sharding import PartitionSpec as P

MESH = pl.DeviceIdType.MESH
ANY = pl.BlockSpec(memory_space=pl.ANY)
F32 = jnp.float32
BF16 = jnp.bfloat16


def flip(ex, mask):
    bit_y = (ex // 4 + mask // 4) % 2
    bit_x = (ex // 2 + mask // 2) % 2
    bit_c = (ex + mask) % 2
    return bit_y * 4 + bit_x * 2 + bit_c


def dot(lhs, rhs, lhs_dim, rhs_dim):
    return lax.dot_general(lhs, rhs, (((lhs_dim,), (rhs_dim,)), ((), ())), preferred_element_type=F32)


AG_KINDS = (
    ((0, 1, 1), (0, 1, 1)),
    ((0, 2, 2), (0, 2, 2)),
    ((0, 4, 4), (0, 4, 4)),
    ((2, 1, 3), (2, 1, 3)),
    ((4, 1, 5), (4, 1, 5)),
    ((2, 4, 6), (4, 2, 6)),
    ((6, 1, 7), (6, 1, 7)),
)
K_OWN_P, K_OWN_X, K_OWN_Y, K_FWD_X, K_FWD_Y, K_DIAG, K_FWD_D = range(7)


def gather_kernel(n_half, n_part, x_ref, dy_ref, g_ref, xall, dyall, gall, own_buf, send_sem, recv_sem, z_send, z_recv, g_send, g_recv, loc_sem):
    st = lax.axis_index("stage")
    ex = lax.axis_index("expert")
    tok = x_ref.shape[0]
    rows_half = tok // n_part
    bar = pltpu.get_barrier_semaphore()

    def block(arr, mask, half):
        start = pl.multiple_of(flip(ex, mask) * tok + half * rows_half, rows_half)
        return arr.at[pl.ds(start, rows_half)]

    def z_copy(half):
        return pltpu.make_async_remote_copy(
            src_ref=x_ref.at[pl.ds(half * rows_half, rows_half)], dst_ref=block(xall, 0, half),
            send_sem=z_send.at[half], recv_sem=z_recv.at[half], device_id=(st + n_half, ex), device_id_type=MESH)

    def zg_copy():
        return pltpu.make_async_remote_copy(
            src_ref=g_ref, dst_ref=gall.at[ex], send_sem=z_send.at[n_part], recv_sem=z_recv.at[n_part],
            device_id=(st + n_half, ex), device_id_type=MESH)

    @pl.when(st < n_half)
    def _():
        pl.semaphore_signal(bar, inc=1, device_id=(st + n_half, ex), device_id_type=MESH)
        pl.semaphore_wait(bar, 1)
        copies = [zg_copy()] + [z_copy(part) for part in range(n_part)]
        for c in copies:
            c.start()
        for c in copies:
            c.wait_send()

    @pl.when(st >= n_half)
    def _():
        pl.semaphore_signal(bar, inc=1, device_id=(st - n_half, ex), device_id_type=MESH)
        for mask in range(1, 8):
            pl.semaphore_signal(bar, inc=1, device_id=(st, flip(ex, mask)), device_id_type=MESH)
        pl.semaphore_wait(bar, 8)

        def copy(arr_id, kind, half, incoming=False):
            arr = (xall, dyall)[arr_id]
            sent, target, got = AG_KINDS[kind][half % 2]
            sem = (arr_id * 7 + kind) * n_part + half
            dst = block(arr, got if incoming else sent, half)
            src = dst
            if sent == 0 and arr_id == 1 and not incoming:
                src = dy_ref.at[pl.ds(half * rows_half, rows_half)]
            return pltpu.make_async_remote_copy(
                src_ref=src, dst_ref=dst, send_sem=send_sem.at[sem], recv_sem=recv_sem.at[sem],
                device_id=(st, flip(ex, target)), device_id_type=MESH)

        def got(arr_id, kind, half):
            copy(arr_id, kind, half, incoming=True).wait_recv()

        def own(arr_id, half):
            for kind in (K_OWN_X, K_OWN_Y, K_OWN_P):
                copy(arr_id, kind, half).start()

        def relay(arr_id, half):
            got(arr_id, K_OWN_X, half)
            if half % 2 == 0:
                copy(arr_id, K_DIAG, half).start()
            copy(arr_id, K_FWD_X, half).start()
            got(arr_id, K_OWN_Y, half)
            if half % 2 == 1:
                copy(arr_id, K_DIAG, half).start()
            copy(arr_id, K_FWD_Y, half).start()

        def diag(arr_id, half):
            got(arr_id, K_DIAG, half)
            copy(arr_id, K_FWD_D, half).start()

        def g_copy(mask, incoming=False):
            idx = flip(ex, mask) if incoming else ex
            return pltpu.make_async_remote_copy(
                src_ref=gall.at[idx], dst_ref=gall.at[idx], send_sem=g_send.at[mask - 1], recv_sem=g_recv.at[mask - 1],
                device_id=(st, flip(ex, mask)), device_id_type=MESH)

        for part in range(n_part):
            own(1, part)
        load = pltpu.make_async_copy(dy_ref, own_buf, loc_sem.at[0])
        load.start()
        load.wait()
        mine = dyall.at[pl.ds(pl.multiple_of(ex * tok, tok), tok)]
        save = pltpu.make_async_copy(own_buf, mine, loc_sem.at[1])
        save.start()
        pltpu.make_async_remote_copy(
            src_ref=gall.at[ex], dst_ref=gall.at[ex], send_sem=z_send.at[n_part], recv_sem=z_recv.at[n_part],
            device_id=(st - n_half, ex), device_id_type=MESH).wait_recv()
        for mask in range(1, 8):
            g_copy(mask).start()

        def x_arrived(half):
            blk = block(xall, 0, half)
            pltpu.make_async_remote_copy(
                src_ref=blk, dst_ref=blk, send_sem=z_send.at[half], recv_sem=z_recv.at[half],
                device_id=(st - n_half, ex), device_id_type=MESH).wait_recv()

        def own_x(part):
            x_arrived(part)
            own(0, part)

        plan = ((relay, 1, 0), (relay, 1, 1), (own_x, 0), (relay, 1, 2), (relay, 1, 3), (diag, 1, 0), (diag, 1, 1), (own_x, 1),
                (relay, 0, 0), (diag, 1, 2), (diag, 1, 3), (own_x, 2), (relay, 0, 1), (diag, 0, 0), (own_x, 3), (relay, 0, 2),
                (diag, 0, 1), (relay, 0, 3), (diag, 0, 2), (diag, 0, 3))
        for act, *where in plan:
            act(*where)
        for arr_id in range(2):
            for half in range(n_part):
                for kind in (K_OWN_P, K_FWD_X, K_FWD_Y, K_FWD_D):
                    got(arr_id, kind, half)
        for mask in range(1, 8):
            g_copy(mask, incoming=True).wait_recv()
        for arr_id in range(2):
            for half in range(n_part):
                for kind in range(7):
                    copy(arr_id, kind, half).wait_send()
        for mask in range(1, 8):
            g_copy(mask).wait_send()
        save.wait()


def main_kernel(n_half, cap, xall, dyall, mrow, mcol, w1, w3, w2, y_out, dx_out, dw1, dw3, dw2, xbuf, qbuf, hbuf, dabuf, dbbuf, sbuf, rbuf,
                w1v, w3v, w2v, xv, dyv, rv, cv, cw, acc, prv, call, ptv, xs, qs, hs, tv, a1, a3, a2,
                w_sem, in_sem, cw_sem, st_sem, acc_sem, pr_sem, send_sem, recv_sem, t_sem, o_sem, dx_send, dx_recv, y_sem):
    st = lax.axis_index("stage")
    ex = lax.axis_index("expert")
    n_loc, d_model, d_ff = w1v.shape
    tok = xv.shape[1]
    tile = tok // 2
    n_blk = rv.shape[0]
    bar = pltpu.get_barrier_semaphore()

    def out_rows(half):
        return call.at[pl.ds(half * tile, tile)]

    def dx_copy(half):
        return pltpu.make_async_remote_copy(
            src_ref=out_rows(half), dst_ref=dx_out.at[pl.ds(half * tile, tile)], send_sem=dx_send.at[half], recv_sem=dx_recv.at[half],
            device_id=(st - n_half, ex), device_id_type=MESH)

    @pl.when(st < n_half)
    def _():
        pl.semaphore_signal(bar, inc=1, device_id=(st + n_half, ex), device_id_type=MESH)
        pl.semaphore_wait(bar, 1)
        for half in range(2):
            view = dx_out.at[pl.ds(half * tile, tile)]
            pltpu.make_async_remote_copy(
                src_ref=view, dst_ref=view, send_sem=dx_send.at[half], recv_sem=dx_recv.at[half],
                device_id=(st + n_half, ex), device_id_type=MESH).wait_recv()

    @pl.when(st >= n_half)
    def _():
        pl.semaphore_signal(bar, inc=1, device_id=(st - n_half, ex), device_id_type=MESH)
        for mask in (1, 2, 4):
            pl.semaphore_signal(bar, inc=1, device_id=(st, flip(ex, mask)), device_id_type=MESH)
        pl.semaphore_wait(bar, 4)

        w_loads = [pltpu.make_async_copy(a, b, w_sem.at[i])
                   for i, (a, b) in enumerate(((mrow, rv), (w1, w1v), (w3, w3v), (w2, w2v)))]
        for c in w_loads:
            c.start()

        def block_rows(k):
            return pl.ds(pl.multiple_of(flip(ex, 7 - k) * tok, tok), tok)

        def col_load(k):
            return pltpu.make_async_copy(mcol.at[block_rows(k)], cv.at[k % 2], in_sem.at[k % 2, 2])

        def x_loads(k):
            slot = k % 2
            return [pltpu.make_async_copy(xall.at[block_rows(k)], xv.at[slot], in_sem.at[slot, 0]),
                    pltpu.make_async_copy(dyall.at[block_rows(k)], dyv.at[slot], in_sem.at[slot, 1]), col_load(k)]

        def pick(meta, slot, half, e):
            rank = meta[slot, half * tile:(half + 1) * tile, e:e + 1]
            return jnp.where(rank == lax.broadcasted_iota(jnp.int32, (tile, cap), 1).astype(F32), 1.0, 0.0).astype(BF16)

        def stores(k, e, buf):
            rows = pl.ds(pl.multiple_of(k * cap, cap), cap)
            mine = pl.ds(pl.multiple_of(buf * cap, cap), cap)
            pairs = [(xs.at[mine], xbuf), (qs.at[mine], qbuf)]
            for i, dst in enumerate((hbuf, dabuf, dbbuf)):
                pairs.append((hs.at[pl.ds(pl.multiple_of((buf * 3 + i) * cap, cap), cap)], dst))
            return [pltpu.make_async_copy(src, dst.at[e, rows], st_sem.at[buf, i]) for i, (src, dst) in enumerate(pairs)]

        def rs_copy(p, k, half):
            mask = 7 - k
            odd = mask % 2 == 1
            slot = jnp.where(odd, (mask // 2) * 2, 6 + mask) + half
            hop = jnp.where(odd, 1, jnp.where(mask == 6, 4 if half else 2, mask))
            return pltpu.make_async_remote_copy(
                src_ref=sbuf.at[p, k, half], dst_ref=rbuf.at[p, slot], send_sem=send_sem.at[p, slot], recv_sem=recv_sem.at[p, slot],
                device_id=(st, flip(ex, hop)), device_id_type=MESH)

        def add_arrived(p, slot, dst):
            view = rbuf.at[p, slot]
            pltpu.make_async_remote_copy(
                src_ref=view, dst_ref=view, send_sem=send_sem.at[p, slot], recv_sem=recv_sem.at[p, slot],
                device_id=(st, flip(ex, 1)), device_id_type=MESH).wait_recv()
            c = pltpu.make_async_copy(view, prv, pr_sem)
            c.start()
            c.wait()

            def add(i, _):
                rows = pl.ds(pl.multiple_of(i * 64, 64), 64)
                acc[dst, rows] = acc[dst, rows] + prv[rows]
                return 0
            lax.fori_loop(0, tile // 64, add, 0)

        def acc_save(p, k, half):
            return pltpu.make_async_copy(acc.at[half], sbuf.at[p, k, half], acc_sem.at[half])

        def finish(p, k, half):
            mask = 7 - k

            @pl.when(mask % 2 == 0)
            def _():
                add_arrived(p, (mask // 2) * 2 + half, half)
            @pl.when(mask == (2 if half else 4))
            def _():
                add_arrived(p, 12 + half, half)
            acc_save(p, k, half).start()

        def send(p, k):
            for half in range(2):
                acc_save(p, k, half).wait()

                @pl.when(k < n_blk - 1)
                def _():
                    rs_copy(p, k, half).start()

        def finalize(p, half, out):
            c = pltpu.make_async_copy(sbuf.at[p, 7, half], acc.at[half], acc_sem.at[half])
            c.start()
            c.wait()
            for mask in (4, 2):
                add_arrived(p, 6 + mask + half, half)
            out[...] = acc[half].astype(BF16)

        def finish_dx(half):
            finalize(0, half, out_rows(half))
            dx_copy(half).start()

        for c in x_loads(0):
            c.start()
        for c in w_loads:
            c.wait()

        def step_one(first, k):
            slot = k % 2
            blk = flip(ex, 7 - k)

            @pl.when(k + 1 < n_blk)
            def _():
                for c in x_loads(k + 1):
                    c.start()
            for c in x_loads(k):
                c.wait()

            def expert(e, _):
                it = k * n_loc + e
                buf = it % 2

                @pl.when(it >= first * n_loc + 2)
                def _():
                    for c in stores(k, e, buf):
                        c.wait()
                rank = rv[blk, pl.ds(e, 1), :]
                gate = rv[blk, pl.ds(e + n_loc, 1), :]
                held = rank == lax.broadcasted_iota(jnp.int32, (cap, tok), 0).astype(F32)
                take = jnp.where(held, 1.0, 0.0).astype(BF16)
                g = jnp.sum(jnp.where(held, gate, 0.0), axis=1, keepdims=True)
                x = dot(take, xv[slot], 1, 0).astype(BF16)
                q = (g * dot(take, dyv[slot], 1, 0)).astype(BF16)
                pre_gate = dot(x, w1v[e], 1, 0)
                pre_up = dot(x, w3v[e], 1, 0)
                dh = dot(q, w2v[e], 1, 1)
                sig = jax.nn.sigmoid(pre_gate)
                act = pre_gate * sig
                da = (dh * pre_up * sig * (1.0 + pre_gate * (1.0 - sig))).astype(BF16)
                db = (dh * act).astype(BF16)
                mine = pl.ds(pl.multiple_of(buf * cap, cap), cap)
                xs[mine, :] = x
                qs[mine, :] = q
                for i, val in enumerate(((act * pre_up).astype(BF16), da, db)):
                    hs[pl.ds(pl.multiple_of((buf * 3 + i) * cap, cap), cap), :] = val
                call[pl.ds(pl.multiple_of(e * cap, cap), cap), :] = (dot(da, w1v[e], 1, 1) + dot(db, w3v[e], 1, 1)).astype(BF16)
                for c in stores(k, e, buf):
                    c.start()
                return 0
            lax.fori_loop(0, n_loc, expert, 0)
            for half in range(2):
                for e in range(n_loc):
                    ptv[:, e * cap:(e + 1) * cap] = pick(cv, slot, half, e)
                acc[half] = dot(ptv[...], call[...], 1, 0)
                finish(0, k, half)

        def h_loads(k):
            rows = pl.ds(pl.multiple_of(k * cap, cap), cap)
            return [pltpu.make_async_copy(hbuf.at[e, rows], tv.at[k % 2, pl.ds(e * cap, cap)], t_sem.at[k % 2, e])
                    for e in range(n_loc)] + [pltpu.make_async_copy(mcol.at[block_rows(k)], cw.at[k % 2], cw_sem.at[k % 2])]

        def step_two(last, k):
            slot = k % 2

            @pl.when(k + 1 < last)
            def _():
                for c in h_loads(k + 1):
                    c.start()
            for c in h_loads(k):
                c.wait()
            for e in range(n_loc):
                out = dot(tv[slot, e * cap:(e + 1) * cap, :], w2v[e], 1, 0).astype(BF16)
                for half in range(2):
                    gate = cw[slot, half * tile:(half + 1) * tile, n_loc + e:n_loc + e + 1]
                    part = gate * dot(pick(cw, slot, half, e), out, 1, 0)
                    acc[half] = part if e == 0 else acc[half] + part
            for half in range(2):
                finish(1, k, half)

        last_one = n_blk + 2
        n_steps = 2 * n_blk

        def plan_of(t):
            early = t < 4
            two = jnp.where(early, t // 2, jnp.where(t < last_one, 0, 1))
            k = jnp.where(early, t % 2, jnp.where(t < last_one, t - 2, t - n_blk))
            return two, k

        def step(t, _):
            two, k = plan_of(t)

            @pl.when(t > 0)
            def _():
                send(*plan_of(t - 1))

            @pl.when(t == last_one + 1)
            def _():
                finish_dx(0)

            @pl.when(two == 0)
            def _():
                step_one(jnp.where(t < 4, 0, 2), k)

            @pl.when((t == 2) | (t == last_one))
            def _():
                for buf in range(2):
                    for c in stores(0, 0, buf):
                        c.wait()
                for c in h_loads(k):
                    c.start()

            @pl.when(two == 1)
            def _():
                step_two(jnp.where(t < 4, 2, n_blk), k)
            return 0
        lax.fori_loop(0, n_steps, step, 0)
        for half in range(2):
            acc_save(1, n_blk - 1, half).wait()

        depth = 2 * cap
        per_e = n_blk // 2

        def d_loads(it):
            e = it // per_e
            slot = it % 2
            rows = pl.ds(pl.multiple_of((it % per_e) * depth, depth), depth)
            top = pl.ds(0, depth)
            return [pltpu.make_async_copy(xbuf.at[e, rows], xv.at[slot, top], in_sem.at[slot, 0]),
                    pltpu.make_async_copy(qbuf.at[e, rows], dyv.at[slot, top], in_sem.at[slot, 1])] + [
                pltpu.make_async_copy(src.at[e, rows], tv.at[slot, pl.ds(i * depth, depth)], t_sem.at[slot, i])
                for i, src in enumerate((hbuf, dabuf, dbbuf))]

        def w_saves(e):
            return [pltpu.make_async_copy(hs.at[pl.ds(0, d_model)], dw1.at[e], o_sem.at[0]),
                    pltpu.make_async_copy(hs.at[pl.ds(d_model, d_model)], dw3.at[e], o_sem.at[1]),
                    pltpu.make_async_copy(qs.at[pl.ds(0, d_ff)], dw2.at[e], o_sem.at[2])]

        for c in d_loads(0):
            c.start()
        total = n_loc * per_e

        def step_three(it, _):
            e = it // per_e
            slot = it % 2

            @pl.when(it + 1 < total)
            def _():
                for c in d_loads(it + 1):
                    c.start()

            @pl.when(it == 1)
            def _():
                finish_dx(1)

            for c in d_loads(it):
                c.wait()

            @pl.when(it % per_e == 0)
            def _():
                a1[...] = jnp.zeros(a1.shape, F32)
                a3[...] = jnp.zeros(a3.shape, F32)
                a2[...] = jnp.zeros(a2.shape, F32)
            x = xv[slot, 0:depth, :]
            a1[...] += dot(x, tv[slot, depth:2 * depth, :], 0, 0)
            a3[...] += dot(x, tv[slot, 2 * depth:3 * depth, :], 0, 0)
            a2[...] += dot(tv[slot, 0:depth, :], dyv[slot, 0:depth, :], 0, 0)

            @pl.when(it % per_e == per_e - 1)
            def _():
                @pl.when(e > 0)
                def _():
                    for c in w_saves(e):
                        c.wait()
                hs[0:d_model, :] = a1[...].astype(BF16)
                hs[d_model:2 * d_model, :] = a3[...].astype(BF16)
                qs[0:d_ff, :] = a2[...].astype(BF16)
                for c in w_saves(e):
                    c.start()
            return 0
        lax.fori_loop(0, total, step_three, 0)

        y_rows = (xs.at[pl.ds(0, tile)], call.at[pl.ds(2 * tile, tile)])

        def y_save(half):
            return pltpu.make_async_copy(y_rows[half], y_out.at[pl.ds(half * tile, tile)], y_sem.at[half])
        for half in range(2):
            finalize(1, half, y_rows[half])
            y_save(half).start()
        for half in range(2):
            dx_copy(half).wait_send()
        for half in range(2):
            y_save(half).wait()
        for c in w_saves(n_loc - 1):
            c.wait()

        def drain(k, _):
            for p in range(2):
                for half in range(2):
                    rs_copy(p, k, half).wait_send()
            return 0
        lax.fori_loop(0, n_blk - 1, drain, 0)


def solution(mesh):
    n_stage = mesh.shape["stage"]
    n_group = mesh.shape["expert"]
    n_half = n_stage // 2
    tok_spec = P("stage", "expert", None)
    w_spec = P("stage", "expert", None, None)

    def device_fn(tokens_in, expert_ids, gate_wts, w_gate, w_up, w_down, grad_out):
        tok, d_model = tokens_in.shape[1:]
        n_loc, _, d_ff = w_gate.shape[1:]
        n_exp = n_loc * n_group
        lane = tok * n_group
        tile = tok // 2
        top_k = expert_ids.shape[2]
        cap = 3 * tok * top_k // (2 * n_exp)
        n_part = 4
        is_b = lax.axis_index("stage") >= n_half
        ex = lax.axis_index("expert")
        ids = expert_ids[0].T[None]
        gate_t = jnp.sum(jnp.where(ids == jnp.arange(n_exp, dtype=jnp.int32)[:, None, None], gate_wts[0].T[None], 0.0), axis=1)

        sds = jax.ShapeDtypeStruct
        dma = pltpu.SemaphoreType.DMA
        xall, dyall, gall = pl.pallas_call(
            functools.partial(gather_kernel, n_half, n_part),
            out_shape=(sds((lane, d_model), BF16), sds((lane, d_model), BF16), sds((n_group, n_exp, tok), F32)),
            in_specs=[ANY] * 3,
            out_specs=(ANY,) * 3,
            scratch_shapes=[pltpu.VMEM((tok, d_model), BF16), dma((14 * n_part,)), dma((14 * n_part,)), dma((n_part + 1,)), dma((n_part + 1,)), dma((7,)), dma((7,)), dma((2,))],
            compiler_params=pltpu.CompilerParams(collective_id=0, has_side_effects=True),
            name="gather_tokens",
        )(tokens_in[0], grad_out[0], gate_t)
        gate_row = lax.dynamic_slice_in_dim(gall, ex * n_loc, n_loc, axis=1)
        held = gate_row > 0.0
        upper = (jnp.arange(tok)[:, None] <= jnp.arange(tok)[None, :]).astype(BF16)
        count = jnp.einsum("set,tu->seu", held.astype(BF16), upper, preferred_element_type=F32)
        mrow = jnp.concatenate([jnp.where(held, count - 1.0, -1.0), gate_row], axis=1)
        mcol = mrow.transpose(0, 2, 1).reshape(lane, 2 * n_loc)

        vm = pltpu.VMEM
        rows = n_group * cap
        outs = pl.pallas_call(
            functools.partial(main_kernel, n_half, cap),
            out_shape=(
                sds((tok, d_model), BF16), sds((tok, d_model), BF16),
                sds((n_loc, d_model, d_ff), BF16), sds((n_loc, d_model, d_ff), BF16), sds((n_loc, d_ff, d_model), BF16),
                sds((n_loc, rows, d_model), BF16), sds((n_loc, rows, d_model), BF16),
                sds((n_loc, rows, d_ff), BF16), sds((n_loc, rows, d_ff), BF16), sds((n_loc, rows, d_ff), BF16),
                sds((2, n_group, 2, tile, d_model), F32), sds((2, 14, tile, d_model), F32)),
            in_specs=[ANY] * 7,
            out_specs=(ANY,) * 12,
            scratch_shapes=[
                vm((n_loc, d_model, d_ff), BF16), vm((n_loc, d_model, d_ff), BF16), vm((n_loc, d_ff, d_model), BF16),
                vm((2, tok, d_model), BF16), vm((2, tok, d_model), BF16), vm((n_group, 2 * n_loc, tok), F32), vm((2, tok, 2 * n_loc), F32),
                vm((2, tok, 2 * n_loc), F32),
                vm((2, tile, d_model), F32), vm((tile, d_model), F32), vm((n_loc * cap, d_model), BF16), vm((tile, n_loc * cap), BF16),
                vm((2 * cap, d_model), BF16), vm((2 * cap, d_model), BF16), vm((6 * cap, d_ff), BF16), vm((2, 6 * cap, d_ff), BF16),
                vm((d_model, d_ff), F32), vm((d_model, d_ff), F32), vm((d_ff, d_model), F32),
                dma((4,)), dma((2, 3)), dma((2,)), dma((2, 5)), dma((2,)), dma, dma((2, 14)), dma((2, 14)),
                dma((2, n_loc)), dma((3,)), dma((2,)), dma((2,)), dma((2,))],
            compiler_params=pltpu.CompilerParams(collective_id=1, has_side_effects=True, vmem_limit_bytes=63 * 1024 * 1024),
            name="experts",
        )(xall, dyall, mrow, mcol, w_gate[0], w_up[0], w_down[0])
        y_local, dx_local, grad_wg, grad_wu, grad_wd = outs[:5]
        on_b = [jnp.where(is_b, v, jnp.zeros_like(v))[None] for v in (y_local, grad_wg, grad_wu, grad_wd)]
        dx_local = jnp.where(is_b, jnp.zeros_like(dx_local), dx_local)
        return on_b[0], dx_local[None], on_b[1], on_b[2], on_b[3]

    return jax.shard_map(device_fn, mesh=mesh, in_specs=(tok_spec, tok_spec, tok_spec, w_spec, w_spec, w_spec, tok_spec), out_specs=(tok_spec, tok_spec, w_spec, w_spec, w_spec), check_vma=False)
```

```python
import functools

import jax
import jax.numpy as jnp
from jax import lax
from jax.experimental import pallas as pl
from jax.experimental.pallas import tpu as pltpu
from jax.sharding import PartitionSpec as P

MESH = pl.DeviceIdType.MESH
ANY = pl.BlockSpec(memory_space=pl.ANY)
F32 = jnp.float32
BF16 = jnp.bfloat16


def flip(ex, mask):
    bit_y = (ex // 4 + mask // 4) % 2
    bit_x = (ex // 2 + mask // 2) % 2
    bit_c = (ex + mask) % 2
    return bit_y * 4 + bit_x * 2 + bit_c


def dot(lhs, rhs, lhs_dim, rhs_dim):
    return lax.dot_general(lhs, rhs, (((lhs_dim,), (rhs_dim,)), ((), ())), preferred_element_type=F32)


AG_KINDS = (
    ((0, 1, 1), (0, 1, 1)),
    ((0, 2, 2), (0, 2, 2)),
    ((0, 4, 4), (0, 4, 4)),
    ((2, 1, 3), (2, 1, 3)),
    ((4, 1, 5), (4, 1, 5)),
    ((2, 4, 6), (4, 2, 6)),
    ((6, 1, 7), (6, 1, 7)),
)
K_OWN_P, K_OWN_X, K_OWN_Y, K_FWD_X, K_FWD_Y, K_DIAG, K_FWD_D = range(7)


def gather_kernel(n_half, n_part, x_ref, dy_ref, g_ref, xall, dyall, gall, own_buf, send_sem, recv_sem, z_send, z_recv, g_send, g_recv, loc_sem):
    st = lax.axis_index("stage")
    ex = lax.axis_index("expert")
    tok = x_ref.shape[0]
    rows_half = tok // n_part
    bar = pltpu.get_barrier_semaphore()

    def block(arr, mask, half):
        start = pl.multiple_of(flip(ex, mask) * tok + half * rows_half, rows_half)
        return arr.at[pl.ds(start, rows_half)]

    def z_copy(half):
        return pltpu.make_async_remote_copy(
            src_ref=x_ref.at[pl.ds(half * rows_half, rows_half)], dst_ref=block(xall, 0, half),
            send_sem=z_send.at[half], recv_sem=z_recv.at[half], device_id=(st + n_half, ex), device_id_type=MESH)

    def zg_copy():
        return pltpu.make_async_remote_copy(
            src_ref=g_ref, dst_ref=gall.at[ex], send_sem=z_send.at[n_part], recv_sem=z_recv.at[n_part],
            device_id=(st + n_half, ex), device_id_type=MESH)

    @pl.when(st < n_half)
    def _():
        pl.semaphore_signal(bar, inc=1, device_id=(st + n_half, ex), device_id_type=MESH)
        pl.semaphore_wait(bar, 1)
        copies = [zg_copy()] + [z_copy(part) for part in range(n_part)]
        for c in copies:
            c.start()
        for c in copies:
            c.wait_send()

    @pl.when(st >= n_half)
    def _():
        pl.semaphore_signal(bar, inc=1, device_id=(st - n_half, ex), device_id_type=MESH)
        for mask in range(1, 8):
            pl.semaphore_signal(bar, inc=1, device_id=(st, flip(ex, mask)), device_id_type=MESH)
        pl.semaphore_wait(bar, 8)

        def copy(arr_id, kind, half, incoming=False):
            arr = (xall, dyall)[arr_id]
            sent, target, got = AG_KINDS[kind][half % 2]
            sem = (arr_id * 7 + kind) * n_part + half
            dst = block(arr, got if incoming else sent, half)
            src = dst
            if sent == 0 and arr_id == 1 and not incoming:
                src = dy_ref.at[pl.ds(half * rows_half, rows_half)]
            return pltpu.make_async_remote_copy(
                src_ref=src, dst_ref=dst, send_sem=send_sem.at[sem], recv_sem=recv_sem.at[sem],
                device_id=(st, flip(ex, target)), device_id_type=MESH)

        def got(arr_id, kind, half):
            copy(arr_id, kind, half, incoming=True).wait_recv()

        def own(arr_id, half):
            for kind in (K_OWN_X, K_OWN_Y, K_OWN_P):
                copy(arr_id, kind, half).start()

        def relay(arr_id, half):
            got(arr_id, K_OWN_X, half)
            if half % 2 == 0:
                copy(arr_id, K_DIAG, half).start()
            copy(arr_id, K_FWD_X, half).start()
            got(arr_id, K_OWN_Y, half)
            if half % 2 == 1:
                copy(arr_id, K_DIAG, half).start()
            copy(arr_id, K_FWD_Y, half).start()

        def diag(arr_id, half):
            got(arr_id, K_DIAG, half)
            copy(arr_id, K_FWD_D, half).start()

        def g_copy(mask, incoming=False):
            idx = flip(ex, mask) if incoming else ex
            return pltpu.make_async_remote_copy(
                src_ref=gall.at[idx], dst_ref=gall.at[idx], send_sem=g_send.at[mask - 1], recv_sem=g_recv.at[mask - 1],
                device_id=(st, flip(ex, mask)), device_id_type=MESH)

        for part in range(n_part):
            own(1, part)
        load = pltpu.make_async_copy(dy_ref, own_buf, loc_sem.at[0])
        load.start()
        load.wait()
        mine = dyall.at[pl.ds(pl.multiple_of(ex * tok, tok), tok)]
        save = pltpu.make_async_copy(own_buf, mine, loc_sem.at[1])
        save.start()
        pltpu.make_async_remote_copy(
            src_ref=gall.at[ex], dst_ref=gall.at[ex], send_sem=z_send.at[n_part], recv_sem=z_recv.at[n_part],
            device_id=(st - n_half, ex), device_id_type=MESH).wait_recv()
        for mask in range(1, 8):
            g_copy(mask).start()

        def x_arrived(half):
            blk = block(xall, 0, half)
            pltpu.make_async_remote_copy(
                src_ref=blk, dst_ref=blk, send_sem=z_send.at[half], recv_sem=z_recv.at[half],
                device_id=(st - n_half, ex), device_id_type=MESH).wait_recv()

        def own_x(part):
            x_arrived(part)
            own(0, part)

        plan = ((relay, 1, 0), (relay, 1, 1), (own_x, 0), (relay, 1, 2), (relay, 1, 3), (diag, 1, 0), (diag, 1, 1), (own_x, 1),
                (relay, 0, 0), (diag, 1, 2), (diag, 1, 3), (own_x, 2), (relay, 0, 1), (diag, 0, 0), (own_x, 3), (relay, 0, 2),
                (diag, 0, 1), (relay, 0, 3), (diag, 0, 2), (diag, 0, 3))
        for act, *where in plan:
            act(*where)
        for arr_id in range(2):
            for half in range(n_part):
                for kind in (K_OWN_P, K_FWD_X, K_FWD_Y, K_FWD_D):
                    got(arr_id, kind, half)
        for mask in range(1, 8):
            g_copy(mask, incoming=True).wait_recv()
        for arr_id in range(2):
            for half in range(n_part):
                for kind in range(7):
                    copy(arr_id, kind, half).wait_send()
        for mask in range(1, 8):
            g_copy(mask).wait_send()
        save.wait()


def main_kernel(n_half, cap, xall, dyall, mrow, mcol, w1, w3, w2, y_out, dx_out, dw1, dw3, dw2, xbuf, qbuf, hbuf, dabuf, dbbuf, sbuf, rbuf,
                w1v, w3v, w2v, xv, dyv, rv, cv, cw, acc, prv, call, ptv, xs, qs, hs, tv, a1, a3, a2,
                w_sem, in_sem, cw_sem, st_sem, acc_sem, pr_sem, send_sem, recv_sem, t_sem, o_sem, dx_send, dx_recv, y_sem):
    st = lax.axis_index("stage")
    ex = lax.axis_index("expert")
    n_loc, d_model, d_ff = w1v.shape
    tok = xv.shape[1]
    tile = tok // 2
    n_blk = rv.shape[0]
    bar = pltpu.get_barrier_semaphore()

    def out_rows(half):
        return call.at[pl.ds(half * tile, tile)]

    def dx_copy(half):
        return pltpu.make_async_remote_copy(
            src_ref=out_rows(half), dst_ref=dx_out.at[pl.ds(half * tile, tile)], send_sem=dx_send.at[half], recv_sem=dx_recv.at[half],
            device_id=(st - n_half, ex), device_id_type=MESH)

    @pl.when(st < n_half)
    def _():
        pl.semaphore_signal(bar, inc=1, device_id=(st + n_half, ex), device_id_type=MESH)
        pl.semaphore_wait(bar, 1)
        for half in range(2):
            view = dx_out.at[pl.ds(half * tile, tile)]
            pltpu.make_async_remote_copy(
                src_ref=view, dst_ref=view, send_sem=dx_send.at[half], recv_sem=dx_recv.at[half],
                device_id=(st + n_half, ex), device_id_type=MESH).wait_recv()

    @pl.when(st >= n_half)
    def _():
        pl.semaphore_signal(bar, inc=1, device_id=(st - n_half, ex), device_id_type=MESH)
        for mask in (1, 2, 4):
            pl.semaphore_signal(bar, inc=1, device_id=(st, flip(ex, mask)), device_id_type=MESH)
        pl.semaphore_wait(bar, 4)

        w_loads = [pltpu.make_async_copy(a, b, w_sem.at[i])
                   for i, (a, b) in enumerate(((mrow, rv), (w1, w1v), (w3, w3v), (w2, w2v)))]
        for c in w_loads:
            c.start()

        def block_rows(k):
            return pl.ds(pl.multiple_of(flip(ex, 7 - k) * tok, tok), tok)

        def col_load(k):
            return pltpu.make_async_copy(mcol.at[block_rows(k)], cv.at[k % 2], in_sem.at[k % 2, 2])

        def x_loads(k):
            slot = k % 2
            return [pltpu.make_async_copy(xall.at[block_rows(k)], xv.at[slot], in_sem.at[slot, 0]),
                    pltpu.make_async_copy(dyall.at[block_rows(k)], dyv.at[slot], in_sem.at[slot, 1]), col_load(k)]

        def pick(meta, slot, half, e):
            rank = meta[slot, half * tile:(half + 1) * tile, e:e + 1]
            return jnp.where(rank == lax.broadcasted_iota(jnp.int32, (tile, cap), 1).astype(F32), 1.0, 0.0).astype(BF16)

        def stores(k, e, buf):
            rows = pl.ds(pl.multiple_of(k * cap, cap), cap)
            mine = pl.ds(pl.multiple_of(buf * cap, cap), cap)
            pairs = [(xs.at[mine], xbuf), (qs.at[mine], qbuf)]
            for i, dst in enumerate((hbuf, dabuf, dbbuf)):
                pairs.append((hs.at[pl.ds(pl.multiple_of((buf * 3 + i) * cap, cap), cap)], dst))
            return [pltpu.make_async_copy(src, dst.at[e, rows], st_sem.at[buf, i]) for i, (src, dst) in enumerate(pairs)]

        def rs_copy(p, k, half):
            mask = 7 - k
            odd = mask % 2 == 1
            slot = jnp.where(odd, (mask // 2) * 2, 6 + mask) + half
            hop = jnp.where(odd, 1, jnp.where(mask == 6, 4 if half else 2, mask))
            return pltpu.make_async_remote_copy(
                src_ref=sbuf.at[p, k, half], dst_ref=rbuf.at[p, slot], send_sem=send_sem.at[p, slot], recv_sem=recv_sem.at[p, slot],
                device_id=(st, flip(ex, hop)), device_id_type=MESH)

        def load_of(p, slot, buf):
            return pltpu.make_async_copy(rbuf.at[p, slot], prv.at[buf], pr_sem.at[buf])

        def fetch(p, slot, buf):
            view = rbuf.at[p, slot]
            pltpu.make_async_remote_copy(
                src_ref=view, dst_ref=view, send_sem=send_sem.at[p, slot], recv_sem=recv_sem.at[p, slot],
                device_id=(st, flip(ex, 1)), device_id_type=MESH).wait_recv()
            load_of(p, slot, buf).start()

        def add_fetched(p, slot, half):
            load_of(p, slot, half).wait()

            def add(i, _):
                rows = pl.ds(pl.multiple_of(i * 64, 64), 64)
                acc[half, rows] = acc[half, rows] + prv[half, rows]
                return 0
            lax.fori_loop(0, tile // 64, add, 0)

        def fetch_partner(p, k):
            mask = 7 - k

            @pl.when(mask % 2 == 0)
            def _():
                for half in range(2):
                    fetch(p, (mask // 2) * 2 + half, half)

        def acc_save(p, k, half):
            return pltpu.make_async_copy(acc.at[half], sbuf.at[p, k, half], acc_sem.at[half])

        def finish(p, k, half):
            mask = 7 - k

            @pl.when(mask % 2 == 0)
            def _():
                add_fetched(p, (mask // 2) * 2 + half, half)
            @pl.when(mask == (2 if half else 4))
            def _():
                fetch(p, 12 + half, half)
                add_fetched(p, 12 + half, half)
            acc_save(p, k, half).start()

        def send(t, half):
            @pl.when(t > 0)
            def _():
                p, k = plan_of(t - 1)
                acc_save(p, k, half).wait()

                @pl.when(k < n_blk - 1)
                def _():
                    rs_copy(p, k, half).start()

        def finalize(p, half, out):
            c = pltpu.make_async_copy(sbuf.at[p, 7, half], acc.at[half], acc_sem.at[half])
            c.start()
            slots = (10 + half, 8 + half)
            for buf, slot in enumerate(slots):
                fetch(p, slot, buf)
            c.wait()
            for buf, slot in enumerate(slots):
                load_of(p, slot, buf).wait()

            def add(i, _):
                rows = pl.ds(pl.multiple_of(i * 64, 64), 64)
                out[rows, :] = (acc[half, rows] + prv[0, rows] + prv[1, rows]).astype(BF16)
                return 0
            lax.fori_loop(0, tile // 64, add, 0)

        def finish_dx(half):
            finalize(0, half, out_rows(half))
            dx_copy(half).start()

        for c in x_loads(0):
            c.start()
        for c in w_loads:
            c.wait()

        def step_one(t, first, k):
            slot = k % 2
            blk = flip(ex, 7 - k)

            @pl.when(k + 1 < n_blk)
            def _():
                for c in x_loads(k + 1):
                    c.start()
            for c in x_loads(k):
                c.wait()

            def expert(e, _):
                it = k * n_loc + e
                buf = it % 2

                @pl.when(e == 1)
                def _():
                    send(t, 1)

                @pl.when(it >= first * n_loc + 2)
                def _():
                    for c in stores(k, e, buf):
                        c.wait()
                rank = rv[blk, pl.ds(e, 1), :]
                gate = rv[blk, pl.ds(e + n_loc, 1), :]
                held = rank == lax.broadcasted_iota(jnp.int32, (cap, tok), 0).astype(F32)
                take = jnp.where(held, 1.0, 0.0).astype(BF16)
                g = jnp.sum(jnp.where(held, gate, 0.0), axis=1, keepdims=True)
                x = dot(take, xv[slot], 1, 0).astype(BF16)
                q = (g * dot(take, dyv[slot], 1, 0)).astype(BF16)
                pre_gate = dot(x, w1v[e], 1, 0)
                pre_up = dot(x, w3v[e], 1, 0)
                dh = dot(q, w2v[e], 1, 1)
                sig = jax.nn.sigmoid(pre_gate)
                act = pre_gate * sig
                da = (dh * pre_up * sig * (1.0 + pre_gate * (1.0 - sig))).astype(BF16)
                db = (dh * act).astype(BF16)
                mine = pl.ds(pl.multiple_of(buf * cap, cap), cap)
                xs[mine, :] = x
                qs[mine, :] = q
                for i, val in enumerate(((act * pre_up).astype(BF16), da, db)):
                    hs[pl.ds(pl.multiple_of((buf * 3 + i) * cap, cap), cap), :] = val
                call[pl.ds(pl.multiple_of(e * cap, cap), cap), :] = (dot(da, w1v[e], 1, 1) + dot(db, w3v[e], 1, 1)).astype(BF16)
                for c in stores(k, e, buf):
                    c.start()
                return 0
            lax.fori_loop(0, n_loc, expert, 0)
            fetch_partner(0, k)
            for half in range(2):
                for e in range(n_loc):
                    ptv[:, e * cap:(e + 1) * cap] = pick(cv, slot, half, e)
                acc[half] = dot(ptv[...], call[...], 1, 0)
                finish(0, k, half)

        def h_loads(k):
            rows = pl.ds(pl.multiple_of(k * cap, cap), cap)
            return [pltpu.make_async_copy(hbuf.at[e, rows], tv.at[k % 2, pl.ds(e * cap, cap)], t_sem.at[k % 2, e])
                    for e in range(n_loc)] + [pltpu.make_async_copy(mcol.at[block_rows(k)], cw.at[k % 2], cw_sem.at[k % 2])]

        def step_two(t, last, k):
            slot = k % 2

            @pl.when(k + 1 < last)
            def _():
                for c in h_loads(k + 1):
                    c.start()
            for c in h_loads(k):
                c.wait()
            for e in range(n_loc):
                out = dot(tv[slot, e * cap:(e + 1) * cap, :], w2v[e], 1, 0).astype(BF16)
                if e == 0:
                    send(t, 1)
                if e == n_loc - 1:
                    fetch_partner(1, k)
                for half in range(2):
                    gate = cw[slot, half * tile:(half + 1) * tile, n_loc + e:n_loc + e + 1]
                    part = gate * dot(pick(cw, slot, half, e), out, 1, 0)
                    acc[half] = part if e == 0 else acc[half] + part
            for half in range(2):
                finish(1, k, half)

        last_one = n_blk + 2
        n_steps = 2 * n_blk

        def plan_of(t):
            early = t < 4
            two = jnp.where(early, t // 2, jnp.where(t < last_one, 0, 1))
            k = jnp.where(early, t % 2, jnp.where(t < last_one, t - 2, t - n_blk))
            return two, k

        def step(t, _):
            two, k = plan_of(t)

            send(t, 0)

            @pl.when(t == last_one + 1)
            def _():
                finish_dx(0)

            @pl.when(two == 0)
            def _():
                step_one(t, jnp.where(t < 4, 0, 2), k)

            @pl.when((t == 2) | (t == last_one))
            def _():
                for buf in range(2):
                    for c in stores(0, 0, buf):
                        c.wait()
                for c in h_loads(k):
                    c.start()

            @pl.when(two == 1)
            def _():
                step_two(t, jnp.where(t < 4, 2, n_blk), k)
            return 0
        lax.fori_loop(0, n_steps, step, 0)
        for half in range(2):
            acc_save(1, n_blk - 1, half).wait()

        depth = 2 * cap
        per_e = n_blk // 2

        def d_loads(it):
            e = it // per_e
            slot = it % 2
            rows = pl.ds(pl.multiple_of((it % per_e) * depth, depth), depth)
            top = pl.ds(0, depth)
            return [pltpu.make_async_copy(xbuf.at[e, rows], xv.at[slot, top], in_sem.at[slot, 0]),
                    pltpu.make_async_copy(qbuf.at[e, rows], dyv.at[slot, top], in_sem.at[slot, 1])] + [
                pltpu.make_async_copy(src.at[e, rows], tv.at[slot, pl.ds(i * depth, depth)], t_sem.at[slot, i])
                for i, src in enumerate((hbuf, dabuf, dbbuf))]

        def w_saves(e):
            return [pltpu.make_async_copy(hs.at[pl.ds(0, d_model)], dw1.at[e], o_sem.at[0]),
                    pltpu.make_async_copy(hs.at[pl.ds(d_model, d_model)], dw3.at[e], o_sem.at[1]),
                    pltpu.make_async_copy(qs.at[pl.ds(0, d_ff)], dw2.at[e], o_sem.at[2])]

        for c in d_loads(0):
            c.start()
        total = n_loc * per_e

        def step_three(it, _):
            e = it // per_e
            slot = it % 2

            @pl.when(it + 1 < total)
            def _():
                for c in d_loads(it + 1):
                    c.start()

            @pl.when(it == 1)
            def _():
                finish_dx(1)

            for c in d_loads(it):
                c.wait()

            @pl.when(it % per_e == 0)
            def _():
                a1[...] = jnp.zeros(a1.shape, F32)
                a3[...] = jnp.zeros(a3.shape, F32)
                a2[...] = jnp.zeros(a2.shape, F32)
            x = xv[slot, 0:depth, :]
            a1[...] += dot(x, tv[slot, depth:2 * depth, :], 0, 0)
            a3[...] += dot(x, tv[slot, 2 * depth:3 * depth, :], 0, 0)
            a2[...] += dot(tv[slot, 0:depth, :], dyv[slot, 0:depth, :], 0, 0)

            @pl.when(it % per_e == per_e - 1)
            def _():
                @pl.when(e > 0)
                def _():
                    for c in w_saves(e):
                        c.wait()
                hs[0:d_model, :] = a1[...].astype(BF16)
                hs[d_model:2 * d_model, :] = a3[...].astype(BF16)
                qs[0:d_ff, :] = a2[...].astype(BF16)
                for c in w_saves(e):
                    c.start()
            return 0
        lax.fori_loop(0, total, step_three, 0)

        y_rows = (xs.at[pl.ds(0, tile)], call.at[pl.ds(2 * tile, tile)])

        def y_save(half):
            return pltpu.make_async_copy(y_rows[half], y_out.at[pl.ds(half * tile, tile)], y_sem.at[half])
        for half in range(2):
            finalize(1, half, y_rows[half])
            y_save(half).start()
        for half in range(2):
            dx_copy(half).wait_send()
        for half in range(2):
            y_save(half).wait()
        for c in w_saves(n_loc - 1):
            c.wait()

        def drain(k, _):
            for p in range(2):
                for half in range(2):
                    rs_copy(p, k, half).wait_send()
            return 0
        lax.fori_loop(0, n_blk - 1, drain, 0)


def solution(mesh):
    n_stage = mesh.shape["stage"]
    n_group = mesh.shape["expert"]
    n_half = n_stage // 2
    tok_spec = P("stage", "expert", None)
    w_spec = P("stage", "expert", None, None)

    def device_fn(tokens_in, expert_ids, gate_wts, w_gate, w_up, w_down, grad_out):
        tok, d_model = tokens_in.shape[1:]
        n_loc, _, d_ff = w_gate.shape[1:]
        n_exp = n_loc * n_group
        lane = tok * n_group
        tile = tok // 2
        top_k = expert_ids.shape[2]
        cap = 3 * tok * top_k // (2 * n_exp)
        n_part = 4
        is_b = lax.axis_index("stage") >= n_half
        ex = lax.axis_index("expert")
        ids = expert_ids[0].T[None]
        gate_t = jnp.sum(jnp.where(ids == jnp.arange(n_exp, dtype=jnp.int32)[:, None, None], gate_wts[0].T[None], 0.0), axis=1)

        sds = jax.ShapeDtypeStruct
        dma = pltpu.SemaphoreType.DMA
        xall, dyall, gall = pl.pallas_call(
            functools.partial(gather_kernel, n_half, n_part),
            out_shape=(sds((lane, d_model), BF16), sds((lane, d_model), BF16), sds((n_group, n_exp, tok), F32)),
            in_specs=[ANY] * 3,
            out_specs=(ANY,) * 3,
            scratch_shapes=[pltpu.VMEM((tok, d_model), BF16), dma((14 * n_part,)), dma((14 * n_part,)), dma((n_part + 1,)), dma((n_part + 1,)), dma((7,)), dma((7,)), dma((2,))],
            compiler_params=pltpu.CompilerParams(collective_id=0, has_side_effects=True),
            name="gather_tokens",
        )(tokens_in[0], grad_out[0], gate_t)
        gate_row = lax.dynamic_slice_in_dim(gall, ex * n_loc, n_loc, axis=1)
        held = gate_row > 0.0
        upper = (jnp.arange(tok)[:, None] <= jnp.arange(tok)[None, :]).astype(BF16)
        count = jnp.einsum("set,tu->seu", held.astype(BF16), upper, preferred_element_type=F32)
        mrow = jnp.concatenate([jnp.where(held, count - 1.0, -1.0), gate_row], axis=1)
        mcol = mrow.transpose(0, 2, 1).reshape(lane, 2 * n_loc)

        vm = pltpu.VMEM
        rows = n_group * cap
        outs = pl.pallas_call(
            functools.partial(main_kernel, n_half, cap),
            out_shape=(
                sds((tok, d_model), BF16), sds((tok, d_model), BF16),
                sds((n_loc, d_model, d_ff), BF16), sds((n_loc, d_model, d_ff), BF16), sds((n_loc, d_ff, d_model), BF16),
                sds((n_loc, rows, d_model), BF16), sds((n_loc, rows, d_model), BF16),
                sds((n_loc, rows, d_ff), BF16), sds((n_loc, rows, d_ff), BF16), sds((n_loc, rows, d_ff), BF16),
                sds((2, n_group, 2, tile, d_model), F32), sds((2, 14, tile, d_model), F32)),
            in_specs=[ANY] * 7,
            out_specs=(ANY,) * 12,
            scratch_shapes=[
                vm((n_loc, d_model, d_ff), BF16), vm((n_loc, d_model, d_ff), BF16), vm((n_loc, d_ff, d_model), BF16),
                vm((2, tok, d_model), BF16), vm((2, tok, d_model), BF16), vm((n_group, 2 * n_loc, tok), F32), vm((2, tok, 2 * n_loc), F32),
                vm((2, tok, 2 * n_loc), F32),
                vm((2, tile, d_model), F32), vm((2, tile, d_model), F32), vm((n_loc * cap, d_model), BF16), vm((tile, n_loc * cap), BF16),
                vm((2 * cap, d_model), BF16), vm((2 * cap, d_model), BF16), vm((6 * cap, d_ff), BF16), vm((2, 6 * cap, d_ff), BF16),
                vm((d_model, d_ff), F32), vm((d_model, d_ff), F32), vm((d_ff, d_model), F32),
                dma((4,)), dma((2, 3)), dma((2,)), dma((2, 5)), dma((2,)), dma((2,)), dma((2, 14)), dma((2, 14)),
                dma((2, n_loc)), dma((3,)), dma((2,)), dma((2,)), dma((2,))],
            compiler_params=pltpu.CompilerParams(collective_id=1, has_side_effects=True, vmem_limit_bytes=63 * 1024 * 1024),
            name="experts",
        )(xall, dyall, mrow, mcol, w_gate[0], w_up[0], w_down[0])
        y_local, dx_local, grad_wg, grad_wu, grad_wd = outs[:5]
        on_b = [jnp.where(is_b, v, jnp.zeros_like(v))[None] for v in (y_local, grad_wg, grad_wu, grad_wd)]
        dx_local = jnp.where(is_b, jnp.zeros_like(dx_local), dx_local)
        return on_b[0], dx_local[None], on_b[1], on_b[2], on_b[3]

    return jax.shard_map(device_fn, mesh=mesh, in_specs=(tok_spec, tok_spec, tok_spec, w_spec, w_spec, w_spec, tok_spec), out_specs=(tok_spec, tok_spec, w_spec, w_spec, w_spec), check_vma=False)
```
